32 devices in a mesh: grp: 2 (over core), row: 16 (over z, y, x).
Axes of the slice: x: 2, y: 2, z: 4, core: 2. Of those that a mesh axis runs over, the one named last changes fastest.
Arguments:
- block_tiles: bfloat16 [256, 2, 128, 128], P(('grp', 'row')), may hold values from -4 to 4
- tile_columns: int32 [256, 2], replicated, may hold values from -1 to 255, as said below
- requests: int32 [32, 32], P(('grp', 'row')), may hold values from -1 to 7, as said below
- output_columns: int32 [256, 2], P(('grp', 'row')), may hold values from 0 to 255, as said below
Outputs:
- product_tiles: bfloat16 [256, 2, 128, 128], P(('grp', 'row'))
The draws below stay inside these ranges and needn't reach their ends.
Inputs may be any that keep to these rules, and one draw needn't show every extreme that they name: `tile_columns`: every block-row has 1 to 2 present tiles (entries >= 0) with different block columns; the data of absent tiles are never read. One device's present tiles number at most 14, exactly 14 on some device in every draw, and name 10 different block columns, at most one block-row of each owner. requests[d, e] is the local index of the block-row of owner e that device d's present tiles name, or -1 where they name none. `output_columns`: the 2 block columns of one block-row differ.
All inputs are finite; a program needn't handle non-finite values.
Results may differ from the reference program's by a relative error of at most 0.001.
Values may be sent and summed in bfloat16 or wider, within the bound.
A program may use at most 128 MiB of HBM per device.

```python
import jax
import jax.numpy as jnp
from jax import lax

TILE = 128
K = 2
P_SIZE = 2
R = 8
OWNERS = 32
ROWS = 256
DISTINCT = 10
LIVE = 14


def build_pattern(key):
    device_ids = jnp.arange(OWNERS, dtype=jnp.int32)
    owner_scores = jax.random.randint(jax.random.fold_in(key, 11), (OWNERS, OWNERS), 0, 65536) * OWNERS + device_ids[None, :]
    named_owner = lax.top_k(owner_scores, DISTINCT)[1].astype(jnp.int32)
    first_pick = jax.random.randint(jax.random.fold_in(key, 12), (OWNERS, OWNERS), 0, R)
    second_pick = jax.random.randint(jax.random.fold_in(key, 13), (OWNERS, OWNERS), 0, R)
    owner_shift = jax.random.randint(jax.random.fold_in(key, 14), (OWNERS,), 0, R)
    pick_row = (first_pick * second_pick // R + owner_shift[None, :]) % R
    named_row = jnp.take_along_axis(pick_row, named_owner, axis=1).astype(jnp.int32)
    named_col = (named_owner * R + named_row).astype(jnp.int32)
    requests = jnp.full((OWNERS, OWNERS), -1, jnp.int32).at[device_ids[:, None], named_owner].set(named_row)
    lowest = max(DISTINCT, R)
    uniform_draw = jax.random.randint(jax.random.fold_in(key, 15), (OWNERS,), 0, 1024)
    counts = lowest + (LIVE - lowest) * uniform_draw * uniform_draw // (1023 * 1023)
    busiest = jax.random.randint(jax.random.fold_in(key, 16), (), 0, OWNERS)
    counts = jnp.where(device_ids == busiest, LIVE, counts).astype(jnp.int32)
    extra_total = counts - R
    spare_slots = R * (K - 1)
    spare_scores = jax.random.randint(jax.random.fold_in(key, 17), (OWNERS, spare_slots), 0, 65536) * spare_slots + jnp.arange(spare_slots, dtype=jnp.int32)[None, :]
    spare_rank = jnp.argsort(jnp.argsort(spare_scores, axis=1), axis=1).astype(jnp.int32)
    spare_live = (spare_rank < extra_total[:, None]).reshape(OWNERS, R, K - 1)
    live_slots = jnp.concatenate([jnp.ones((OWNERS, R, 1), bool), spare_live], axis=2)
    row_shift = jax.random.randint(jax.random.fold_in(key, 18), (OWNERS, R, 1), 0, K)
    rotate_index = (jnp.arange(K, dtype=jnp.int32)[None, None, :] + row_shift) % K
    live_slots = jnp.take_along_axis(live_slots, rotate_index, axis=2).reshape(OWNERS, R * K)
    live_order = jnp.cumsum(live_slots.astype(jnp.int32), axis=1) - 1
    cycled = jnp.take_along_axis(named_col, jnp.maximum(live_order, 0) % DISTINCT, axis=1)
    tile_columns = jnp.where(live_slots, cycled, -1).reshape(ROWS, K).astype(jnp.int32)
    safe_cols = jnp.maximum(tile_columns, 0)
    right_cols = tile_columns[safe_cols]
    candidate_live = (tile_columns >= 0)[:, :, None] & (right_cols >= 0)
    candidates = right_cols.reshape(ROWS, K * K)
    candidate_live = candidate_live.reshape(ROWS, K * K).astype(jnp.int32)
    noise_draw = jax.random.randint(jax.random.fold_in(key, 19), (ROWS, K * K), 0, 65536)
    scores = candidate_live * 67108864 + noise_draw * 16 + jnp.arange(K * K, dtype=jnp.int32)[None, :]
    first_place = lax.top_k(scores, 1)[1][:, 0]
    first_col = jnp.take_along_axis(candidates, first_place[:, None], axis=1)[:, 0]
    second_scores = jnp.where(candidates == first_col[:, None], -1, scores)
    second_value, second_place = lax.top_k(second_scores, 1)
    second_live = second_value[:, 0] >= 67108864
    fallback = (first_col + 1 + jax.random.randint(jax.random.fold_in(key, 20), (ROWS,), 0, ROWS - 1)) % ROWS
    second_col = jnp.where(second_live, jnp.take_along_axis(candidates, second_place, axis=1)[:, 0], fallback)
    output_columns = jnp.stack([first_col, second_col], axis=1).astype(jnp.int32)
    return (tile_columns, requests, output_columns)


def draw_tile_columns(key, part):
    return build_pattern(key)[0]


def draw_requests(key, part):
    return build_pattern(key)[1]


def draw_output_columns(key, part):
    return build_pattern(key)[2]


def block_levels(key, dims, cuts, least, largest):
    loudness = 1.0
    for position, parts in cuts:
        steps = jax.random.uniform(jax.random.fold_in(jax.random.fold_in(key, 6), position), (parts,), jnp.float32, least / len(cuts), largest / len(cuts))
        loudness = loudness * jnp.repeat(jnp.exp(steps), dims[position] // parts).reshape((-1,) + (1,) * (len(dims) - 1 - position))
    return loudness


def gaussian(rng, extent, width, limit, cuts=(), kind=jnp.bfloat16):
    result = jax.random.normal(rng, extent, jnp.float32) * width
    if len(cuts) > 0:
        result = block_levels(rng, extent, cuts, -0.22, 0.18) * result
    return jnp.clip(result, min=-limit, max=limit).astype(kind)


def setup_inputs(seed: int = 0) -> dict:
    key_of = jax.random.split(jax.random.key(seed), 5)
    block_tiles = gaussian(key_of[0], (ROWS, K, TILE, TILE), 0.3, 4.0, ((0, 32),))
    tile_columns = draw_tile_columns(jax.random.fold_in(key_of[4], 71), 0)
    requests = draw_requests(jax.random.fold_in(key_of[4], 71), 0)
    output_columns = draw_output_columns(jax.random.fold_in(key_of[4], 71), 0)
    return dict(block_tiles=block_tiles, tile_columns=tile_columns, requests=requests, output_columns=output_columns)


def block_terms(tiles_left, cols_left, outs_left, received, recv_cols):
    present = cols_left >= 0
    owner_slot = jnp.where(present, cols_left // R, 0).astype(jnp.int32)
    right_tiles = received[owner_slot].astype(jnp.float32)
    right_cols = recv_cols[owner_slot]
    products = jnp.einsum("gkab,gkjbc->gkjac", tiles_left.astype(jnp.float32), right_tiles)
    select = (right_cols[:, None, :, :] == outs_left[:, :, None, None]) & present[:, None, :, None]
    weights = jnp.where(select, jnp.ones((), jnp.float32), jnp.zeros((), jnp.float32))
    return jnp.einsum("gpkj,gkjac->gpac", weights, products, precision=lax.Precision.HIGHEST)


def device_result(device, block_tiles, tile_columns, requests, output_columns):
    asked = requests[device]
    present_ask = asked >= 0
    source_rows = (jnp.arange(OWNERS, dtype=jnp.int32) * R + jnp.maximum(asked, 0)).astype(jnp.int32)
    received = jnp.where(present_ask[:, None, None, None], block_tiles[source_rows], jnp.zeros((), jnp.bfloat16))
    recv_cols = jnp.where(present_ask[:, None], tile_columns[source_rows], -1).astype(jnp.int32)
    start_row = (device * R).astype(jnp.int32)
    own_tiles = lax.dynamic_slice_in_dim(block_tiles, start_row, R, 0).reshape(R // 8, 8, K, TILE, TILE)
    own_cols = lax.dynamic_slice_in_dim(tile_columns, start_row, R, 0).reshape(R // 8, 8, K)
    own_outs = lax.dynamic_slice_in_dim(output_columns, start_row, R, 0).reshape(R // 8, 8, P_SIZE)

    def one_block(pieces):
        return block_terms(pieces[0], pieces[1], pieces[2], received, recv_cols)

    merged = lax.map(one_block, (own_tiles, own_cols, own_outs))
    return merged.reshape(R, P_SIZE, TILE, TILE).astype(jnp.bfloat16)


def reference(block_tiles, tile_columns, requests, output_columns):
    def one_device(device):
        return device_result(device, block_tiles, tile_columns, requests, output_columns)

    results = lax.map(one_device, jnp.arange(OWNERS, dtype=jnp.int32))
    return results.reshape(ROWS, P_SIZE, TILE, TILE)
```

```python
import functools

import jax
import jax.numpy as jnp
from jax import lax
from jax.experimental import pallas as pl
from jax.experimental.pallas import tpu as pltpu
from jax.sharding import PartitionSpec as P

MESH = pl.DeviceIdType.MESH
PLANE = 4
CUT_B = (4, 18)
CAP_B = 32
CUT_C = (4,)
CAP_C = 21


def multiply(base, find, cols_ref, outs_ref, tiles_ref, rbuf, out_ref):
    rows, per_row, side, _ = tiles_ref.shape
    outs_row = outs_ref.shape[0]
    for i in range(rows):
        left = jnp.concatenate([tiles_ref[i, k] for k in range(per_row)], axis=1)
        stack = []
        for k in range(per_row):
            c = cols_ref[k, base + i]
            safe = jnp.maximum(c, 0)
            slot = find(safe // rows)
            line = []
            for p in range(outs_row):
                o = outs_ref[p, i]
                which = jnp.int32(0)
                hit = jnp.int32(0)
                for j in range(per_row):
                    same = cols_ref[j, safe] == o
                    which = jnp.where(same, j, which)
                    hit = jnp.where(same & (c >= 0), 1, hit)
                tile = rbuf[slot, which]
                line.append(tile * hit.astype(jnp.float32).astype(jnp.bfloat16))
            stack.append(jnp.concatenate(line, axis=1))
        right = jnp.concatenate(stack, axis=0)
        prod = jnp.dot(left, right, preferred_element_type=jnp.float32).astype(jnp.bfloat16)
        for p in range(outs_row):
            out_ref[i, p] = prod[:, p * side : (p + 1) * side]


def dense_kernel(
    groups, members, cols_ref, outs_ref, tiles_ref, out_ref,
    sbuf, rbuf, mbuf, send_sem, recv_sem, mirror_send, mirror_recv,
):
    part = members // 2
    n = groups * part
    rows, per_row, side, _ = tiles_ref.shape
    grp, row = lax.axis_index("grp"), lax.axis_index("row")
    half, spot = row // part, lax.rem(row, part)
    me = grp * part + spot
    base = (grp * members + row) * rows
    mirror_row = (1 - half) * part + spot
    mirror = {"grp": grp, "row": mirror_row}
    mirror_base = (grp * members + mirror_row) * rows

    def place(s):
        u = lax.rem(me + s, n)
        return u // part, half * part + lax.rem(u, part)

    def target(s):
        g, r = place(s)
        return {"grp": g, "row": r}

    barrier = pltpu.get_barrier_semaphore()
    pl.semaphore_signal(barrier, inc=1, device_id=mirror, device_id_type=MESH)

    def greet(s, carry):
        pl.semaphore_signal(barrier, inc=1, device_id=target(s), device_id_type=MESH)
        return carry

    lax.fori_loop(1, n, greet, 0)

    def asked(s, start):
        g, r = place(s)
        first = (g * members + r) * rows
        t = jnp.int32(0)
        for i in range(rows):
            for k in range(per_row):
                c = cols_ref[k, first + i] - start
                t = jnp.where((c >= 0) & (c < rows), c, t)
        return t

    def copy(s, level):
        return pltpu.make_async_remote_copy(
            src_ref=sbuf.at[level * n + s],
            dst_ref=rbuf.at[level * n + s],
            send_sem=send_sem.at[level * n + s],
            recv_sem=recv_sem.at[level * n + s],
            device_id=target(s),
            device_id_type=MESH,
        )

    def pack(s, carry):
        sbuf[s] = tiles_ref[asked(s, base)]
        return carry

    lax.fori_loop(1, n, pack, 0)
    pl.semaphore_wait(barrier, n)
    across = pltpu.make_async_remote_copy(
        src_ref=tiles_ref,
        dst_ref=mbuf,
        send_sem=mirror_send,
        recv_sem=mirror_recv,
        device_id=mirror,
        device_id_type=MESH,
    )
    across.start()

    def send(s, carry):
        copy(s, 0).start()
        return carry

    lax.fori_loop(1, n, send, 0)
    rbuf[0] = tiles_ref[asked(0, base)]
    across.wait()

    def relay(s, carry):
        sbuf[n + s] = mbuf[asked(s, mirror_base)]
        return carry

    lax.fori_loop(1, n, relay, 0)

    def forward(s, carry):
        copy(s, 1).start()
        return carry

    lax.fori_loop(1, n, forward, 0)
    rbuf[n] = mbuf[asked(0, mirror_base)]

    def land(s, carry):
        copy(s, 0).wait()
        copy(s, 1).wait()
        return carry

    lax.fori_loop(1, n, land, 0)

    def find(owner):
        owner_row = lax.rem(owner, members)
        spot_of = owner // members * part + lax.rem(owner_row, part)
        return lax.rem(me - spot_of + n, n) + jnp.where(owner_row // part == half, 0, n)

    multiply(base, find, cols_ref, outs_ref, tiles_ref, rbuf, out_ref)


def same(lane, rows, groups, members):
    device = lane // rows
    inner = lax.rem(device, members)
    spot = lax.rem(inner, PLANE)
    return device // members, inner // PLANE, spot // 2, lax.rem(spot, 2)


def level(rel):
    spot = lax.rem(rel, PLANE)
    return jnp.where(spot == 0, 0, jnp.where(spot == PLANE - 1, 2, 1))


def ones(mask):
    return jnp.where(mask, 1.0, 0.0)


def across(a, b):
    dims = (((1,), (1,)), ((), ()))
    return lax.dot_general(
        a.astype(jnp.bfloat16), b.astype(jnp.bfloat16), dims, preferred_element_type=jnp.float32
    )


def iota(shape, axis):
    return lax.broadcasted_iota(jnp.int32, shape, axis)


def named_rows(cols, here, rows, groups, members):
    g, z, y, x = here
    lines = members // PLANE
    total = cols.shape[1]
    devices = groups * members
    count = devices + 16
    query = iota((count, total), 0)
    lane = iota((count, total), 1)
    og, oz, oy, ox = same(lane, rows, groups, members)
    rel = PLANE * lax.rem(og + g, 2) + 2 * lax.rem(oy + y, 2) + lax.rem(ox + x, 2)
    step = query - devices
    alone = (step < 0) & (lane // rows == query)
    plane = (step >= 0) & (step < lines) & (oz == lax.rem(z + jnp.maximum(step, 0), lines))
    near = (oz == z) & (rel == step - 8)
    group = ones(alone | plane | near)
    index = iota((total, total), 0)
    hits = jnp.zeros((count, total), jnp.float32)
    for k in range(cols.shape[0]):
        hits = hits + across(group, ones(index == cols[k : k + 1]))
    return ones(hits > 0.5)


def tables(cols, named, here, rows, groups, members):
    g, z, y, x = here
    lines = members // PLANE
    devices = groups * members
    total = cols.shape[1]
    per = cols.shape[0]
    lane = iota((8, total), 1)
    sub = iota((8, total), 0)
    og, oz, oy, ox = same(lane, rows, groups, members)
    rel = PLANE * lax.rem(og + g, 2) + 2 * lax.rem(oy + y, 2) + lax.rem(ox + x, 2)
    lev = level(rel)
    local = oz == z
    back = lax.rem(z - oz + lines, lines)
    planes = named[devices : devices + 8]
    mine = jnp.broadcast_to(planes[0:1], (8, total))
    near = named[devices + 8 : devices + 16]
    sends = [planes * ones(local & (lev == k)) for k in range(3)]
    takes = [mine * ones((back == sub) & (lev == k)) for k in range(3)]
    mids = [near * ones(local), near * ones(~local)]
    stack = jnp.concatenate(sends + takes + mids, axis=0)
    upper = ones(iota((total, total), 0) > iota((total, total), 1))
    masks, ranks = [], []
    before = jnp.zeros((stack.shape[0], 1), jnp.float32)
    for j in range(per):
        m = stack * ones(cols[j : j + 1] >= 0)
        ranks.append(across(m, upper) + before)
        masks.append(m)
        before = before + jnp.sum(m, axis=1, keepdims=True)

    def slots(first, bounds):
        parts = range(first, first + len(bounds))
        sums = [before[8 * b : 8 * b + 8] for b in parts]
        start = jnp.zeros((8, 1), jnp.float32)
        where = []
        used = [jnp.zeros((8, total), jnp.float32) for j in range(per)]
        at = [jnp.zeros((8, total), jnp.float32) for j in range(per)]
        for b, bound, n in zip(parts, bounds, sums):
            start = jnp.maximum(start, bound)
            for j in range(per):
                m = masks[j][8 * b : 8 * b + 8]
                used[j] = used[j] + m
                at[j] = at[j] + m * (start + ranks[j][8 * b : 8 * b + 8])
            start = start + n
        return used, at

    send_used, send_at = slots(0, (0.0, CUT_B[0], CUT_B[1]))
    take_used, take_at = slots(3, (0.0, CUT_B[0], CUT_B[1]))
    mid_used, mid_at = slots(6, (0.0, CUT_C[0]))
    item = lax.rem(lane, rows)
    held = groups * PLANE * rows * per
    home = [(rel * (rows * per) + item * per + j).astype(jnp.float32) for j in range(per)]
    offset = (held + (sub - 1) * CAP_B).astype(jnp.float32)
    arrived = []
    for j in range(per):
        far = jnp.sum(take_used[j] * (offset + jnp.minimum(take_at[j], CAP_B - 1.0)), axis=0, keepdims=True)
        arrived.append(jnp.where(local, home[j], jnp.broadcast_to(far, (8, total))))

    def sources(used, at, address, first, count):
        out = jnp.zeros((8, 32 * count), jnp.float32)
        slot = iota((32, total), 0)
        for j in range(per):
            spot = jnp.where(used[j] > 0.5, at[j], -1.0).astype(jnp.int32)
            hot = jnp.concatenate(
                [ones(slot == spot[first + q : first + q + 1]) for q in range(count)], axis=0
            )
            out = out + across(address[j], hot)
        return jnp.clip(out.astype(jnp.int32), 0, held + (lines - 1) * CAP_B - 1)

    b_list = sources(send_used, send_at, home, 0, lines)
    c_list = sources(mid_used, mid_at, arrived, 0, groups * PLANE)
    final = [jnp.clip(mid_at[j][0:1].astype(jnp.int32), 0, CAP_C - 1) for j in range(per)]
    lines_out = [b_list[0:1, :128], c_list[0:1, :128], c_list[0:1, 128:256]]
    for j in range(per):
        for h in range(total // 128):
            lines_out.append(final[j][:, 128 * h : 128 * h + 128])
    lines_out.append(jnp.zeros((1, 128), jnp.int32))
    return jnp.concatenate(lines_out, axis=0)


def overflow(cols, named, here, rows, groups, members):
    g, z, y, x = here
    lines = members // PLANE
    devices = groups * members
    total = cols.shape[1]
    count = sum(ones(cols[j : j + 1] >= 0) for j in range(cols.shape[0]))
    lane = iota((devices, total), 1)
    row = iota((devices, total), 0)
    local = lax.rem(row, members) // PLANE == lax.rem(lane // rows, members) // PLANE
    load = named[:devices] * count
    inner = jnp.sum(load * ones(local), axis=1, keepdims=True)
    outer = jnp.sum(load * ones(~local), axis=1, keepdims=True)
    over = jnp.max(jnp.maximum(inner, CUT_C[0]) + outer - CAP_C)
    owner = ones(iota((128, total), 0) == iota((128, total), 1) // rows)
    by_owner = across(named[devices : devices + 8] * count, owner)
    at = iota((128, 128), 0)
    of = iota((128, 128), 1)
    ag, az, ay, ax = same(at, 1, groups, members)
    og, oz, oy, ox = same(of, 1, groups, members)
    rel = PLANE * lax.rem(og + ag, 2) + 2 * lax.rem(oy + ay, 2) + lax.rem(ox + ax, 2)
    valid = (az == oz) & (at < devices) & (of < devices)
    start = jnp.zeros((8, 128), jnp.float32)
    for k, bound in enumerate((0.0, CUT_B[0], CUT_B[1])):
        start = jnp.maximum(start, bound)
        start = start + across(by_owner, ones(valid & (level(rel) == k)))
    sub = iota((8, 128), 0)
    source = lax.rem(iota((8, 128), 1), members) // PLANE
    counted = (sub < lines) & (source != lax.rem(z + sub, lines))
    return jnp.maximum(over, jnp.max(jnp.where(counted, start - CAP_B, 0.0))).astype(jnp.int32)


def compact_kernel(
    groups, members, cols_ref, outs_ref, cols_vec, tiles_hbm, out_ref, over_ref,
    tiles, parts, arena, b_send, b_recv, c_send, c_recv, tab_vec, tab,
    load_sem, tab_sem, a_out, a_in, b_out, b_in, c_out, c_in,
):
    rows, per, side, _ = tiles.shape
    lines = members // PLANE
    crowd = groups * PLANE
    piece = side // crowd
    g, row = lax.axis_index("grp"), lax.axis_index("row")
    z, spot = row // PLANE, lax.rem(row, PLANE)
    y, x = spot // 2, lax.rem(spot, 2)
    here = (g, z, y, x)
    base = (g * members + row) * rows
    me = g * PLANE + spot

    def near(u):
        dg, dy, dx = u // PLANE, u // 2 % 2, u % 2
        return lax.rem(g + dg, 2), 2 * lax.rem(y + dy, 2) + lax.rem(x + dx, 2)

    def near_device(u):
        ng, ns = near(u)
        return {"grp": ng, "row": z * PLANE + ns}

    def line_device(dz):
        return {"grp": g, "row": lax.rem(z + dz, lines) * PLANE + spot}

    load = pltpu.make_async_copy(tiles_hbm, tiles, load_sem)
    load.start()
    barrier = pltpu.get_barrier_semaphore()
    for dz in range(1, lines):
        pl.semaphore_signal(barrier, inc=1, device_id=line_device(dz), device_id_type=MESH)
    for u in range(1, crowd):
        pl.semaphore_signal(barrier, inc=1, device_id=near_device(u), device_id_type=MESH)

    cols = cols_vec[...]
    named = named_rows(cols, here, rows, groups, members)
    tab_vec[...] = tables(cols, named, here, rows, groups, members)
    move = pltpu.make_async_copy(tab_vec, tab, tab_sem)
    move.start()
    load.wait()
    pl.semaphore_wait(barrier, lines - 1 + crowd - 1)

    def a_copy(u):
        ng, ns = near(u)
        start = pl.multiple_of((ng * PLANE + ns) * piece, piece)
        return pltpu.make_async_remote_copy(
            src_ref=tiles.at[:, :, pl.ds(start, piece), :],
            dst_ref=parts.at[u],
            send_sem=a_out.at[u],
            recv_sem=a_in.at[u],
            device_id=near_device(u),
            device_id_type=MESH,
        )

    order = [4, 1, 2, 5, 6, 3, 7]
    for u in order:
        a_copy(u).start()

    def settle(u):
        for i in range(rows):
            for j in range(per):
                arena[(u * rows + i) * per + j] = parts[u, i, j]

    mine = pl.multiple_of(me * piece, piece)
    for i in range(rows):
        for j in range(per):
            arena[i * per + j] = tiles[i, j, pl.ds(mine, piece), :]
    move.wait()

    cuts_b = (0,) + CUT_B + (CAP_B,)
    cuts_c = (0,) + CUT_C + (CAP_C,)

    def b_copy(k, dz):
        span = pl.ds(cuts_b[k], cuts_b[k + 1] - cuts_b[k])
        return pltpu.make_async_remote_copy(
            src_ref=b_send.at[dz - 1, span],
            dst_ref=b_recv.at[dz - 1, span],
            send_sem=b_out.at[3 * (dz - 1) + k],
            recv_sem=b_in.at[3 * (dz - 1) + k],
            device_id=line_device(dz),
            device_id_type=MESH,
        )

    def c_copy(k, u):
        span = pl.ds(cuts_c[k], cuts_c[k + 1] - cuts_c[k])
        return pltpu.make_async_remote_copy(
            src_ref=c_send.at[u, span],
            dst_ref=c_recv.at[u, span],
            send_sem=c_out.at[2 * u + k],
            recv_sem=c_in.at[2 * u + k],
            device_id=near_device(u),
            device_id_type=MESH,
        )

    def push_b(k):
        for dz in range(1, lines):
            for q in range(cuts_b[k], cuts_b[k + 1]):
                b_send[dz - 1, q] = arena[tab[0, 32 * dz + q]]
            b_copy(k, dz).start()

    def push_c(k):
        for u in order + [0]:
            for q in range(cuts_c[k], cuts_c[k + 1]):
                tile = arena[tab[1 + u // 4, 32 * (u % 4) + q]]
                if u:
                    c_send[u, q] = tile
                else:
                    c_recv[0, q] = tile
            if u:
                c_copy(k, u).start()

    a_copy(4).wait_recv()
    settle(4)
    push_b(0)
    over_ref[0] = overflow(cols, named, here, rows, groups, members)
    for u in (1, 2, 5, 6):
        a_copy(u).wait_recv()
        settle(u)
    push_b(1)
    for u in (3, 7):
        a_copy(u).wait_recv()
        settle(u)
    push_b(2)
    push_c(0)
    held = crowd * rows * per
    for k in range(3):
        for dz in range(1, lines):
            b_copy(k, dz).wait_recv()
            for q in range(cuts_b[k], cuts_b[k + 1]):
                arena[held + (dz - 1) * CAP_B + q] = b_recv[dz - 1, q]
    push_c(1)

    sources = []
    for piece_of in range(crowd):
        pg, ps = piece_of // PLANE, piece_of % PLANE
        dy, dx = lax.rem(ps // 2 + y, 2), lax.rem(ps % 2 + x, 2)
        sources.append(PLANE * lax.rem(pg + g, 2) + 2 * dy + dx)
    for u in range(1, crowd):
        for k in range(2):
            c_copy(k, u).wait_recv()

    outs_row = outs_ref.shape[0]
    wide = cols_ref.shape[1] // 128
    for i in range(rows):
        left = jnp.concatenate([tiles[i, k] for k in range(per)], axis=1)
        stack = []
        for k in range(per):
            c = cols_ref[k, base + i]
            safe = jnp.maximum(c, 0)
            line = []
            for p in range(outs_row):
                o = outs_ref[p, i]
                which = jnp.int32(0)
                hit = jnp.int32(0)
                for j in range(per):
                    match = cols_ref[j, safe] == o
                    which = jnp.where(match, j, which)
                    hit = jnp.where(match & (c >= 0), 1, hit)
                slot = tab[3 + wide * which + safe // 128, lax.rem(safe, 128)]
                tile = jnp.concatenate([c_recv[s, slot] for s in sources], axis=0)
                line.append(tile * hit.astype(jnp.float32).astype(jnp.bfloat16))
            stack.append(jnp.concatenate(line, axis=1))
        right = jnp.concatenate(stack, axis=0)
        prod = jnp.dot(left, right, preferred_element_type=jnp.float32).astype(jnp.bfloat16)
        for p in range(outs_row):
            out_ref[i, p] = prod[:, p * side : (p + 1) * side]

    for u in range(1, crowd):
        a_copy(u).wait_send()
        for k in range(2):
            c_copy(k, u).wait_send()
    for dz in range(1, lines):
        for k in range(3):
            b_copy(k, dz).wait_send()


def params(identity):
    return pltpu.CompilerParams(
        collective_id=identity, has_side_effects=True, vmem_limit_bytes=56 * 1024 * 1024
    )


def shards(block_tiles, tile_columns, requests, output_columns):
    groups = lax.axis_size("grp")
    members = lax.axis_size("row")
    n = groups * members
    rows, per_row, side, _ = block_tiles.shape
    vmem = pl.BlockSpec(memory_space=pltpu.VMEM)
    smem = pl.BlockSpec(memory_space=pltpu.SMEM)
    out = jax.ShapeDtypeStruct((rows, output_columns.shape[1], side, side), jnp.bfloat16)
    tile_rows = lambda count: pltpu.VMEM((count, per_row, side, side), jnp.bfloat16)
    columns, outs = tile_columns.T, output_columns.T

    def dense():
        return pl.pallas_call(
            functools.partial(dense_kernel, groups, members),
            out_shape=out,
            in_specs=[smem, smem, vmem],
            out_specs=vmem,
            scratch_shapes=[
                tile_rows(n),
                tile_rows(n),
                tile_rows(rows),
                pltpu.SemaphoreType.DMA((n,)),
                pltpu.SemaphoreType.DMA((n,)),
                pltpu.SemaphoreType.DMA,
                pltpu.SemaphoreType.DMA,
            ],
            compiler_params=params(0),
        )(columns, outs, block_tiles)

    lines = members // PLANE
    crowd = groups * PLANE
    held = crowd * rows * per_row + (lines - 1) * CAP_B
    fits = groups == 2 and members == lines * PLANE and lines <= 4 and per_row == 2
    fits = fits and tile_columns.shape[0] == 256 and side % (16 * crowd) == 0 and held <= 256
    if not fits:
        return dense()
    piece = side // crowd
    pieces = lambda *lead: pltpu.VMEM((*lead, piece, side), jnp.bfloat16)
    dma = pltpu.SemaphoreType.DMA
    compact, over = pl.pallas_call(
        functools.partial(compact_kernel, groups, members),
        out_shape=(out, jax.ShapeDtypeStruct((1,), jnp.int32)),
        in_specs=[smem, smem, vmem, pl.BlockSpec(memory_space=pl.ANY)],
        out_specs=(vmem, smem),
        scratch_shapes=[
            pltpu.VMEM(block_tiles.shape, jnp.bfloat16),
            pieces(crowd, rows, per_row),
            pieces(held),
            pieces(lines - 1, CAP_B),
            pieces(lines - 1, CAP_B),
            pieces(crowd, CAP_C),
            pieces(crowd, CAP_C),
            pltpu.VMEM((8, 128), jnp.int32),
            pltpu.SMEM((8, 128), jnp.int32),
            dma,
            dma,
            dma((crowd,)),
            dma((crowd,)),
            dma((3 * (lines - 1),)),
            dma((3 * (lines - 1),)),
            dma((2 * crowd,)),
            dma((2 * crowd,)),
        ],
        compiler_params=params(1),
    )(columns, outs, columns, block_tiles)
    return lax.cond(over[0] > 0, dense, lambda: compact)


def solution(mesh):
    placed = (
        P(("grp", "row"), None, None, None),
        P(),
        P(("grp", "row"), None),
        P(("grp", "row"), None),
    )
    return jax.shard_map(
        shards,
        mesh=mesh,
        in_specs=placed,
        out_specs=P(("grp", "row"), None, None, None),
        check_vma=False,
    )
```

```python
import functools

import jax
import jax.numpy as jnp
from jax import lax
from jax.experimental import pallas as pl
from jax.experimental.pallas import tpu as pltpu
from jax.sharding import PartitionSpec as P

MESH = pl.DeviceIdType.MESH
PLANE = 4
ROW_CUT = (1, 3)
CUT_B = (0, 2, 8, 22, 33)
PART_B = (8, 22)
CUT_C = (0, 3, 7, 17, 22)
SPAN = 40
TABLE = 16


def multiply(base, find, cols_ref, outs_ref, tiles_ref, rbuf, out_ref):
    rows, per_row, side, _ = tiles_ref.shape
    outs_row = outs_ref.shape[0]
    for i in range(rows):
        left = jnp.concatenate([tiles_ref[i, k] for k in range(per_row)], axis=1)
        stack = []
        for k in range(per_row):
            c = cols_ref[k, base + i]
            safe = jnp.maximum(c, 0)
            slot = find(safe // rows)
            line = []
            for p in range(outs_row):
                o = outs_ref[p, i]
                which = jnp.int32(0)
                hit = jnp.int32(0)
                for j in range(per_row):
                    same = cols_ref[j, safe] == o
                    which = jnp.where(same, j, which)
                    hit = jnp.where(same & (c >= 0), 1, hit)
                tile = rbuf[slot, which]
                line.append(tile * hit.astype(jnp.float32).astype(jnp.bfloat16))
            stack.append(jnp.concatenate(line, axis=1))
        right = jnp.concatenate(stack, axis=0)
        prod = jnp.dot(left, right, preferred_element_type=jnp.float32).astype(jnp.bfloat16)
        for p in range(outs_row):
            out_ref[i, p] = prod[:, p * side : (p + 1) * side]


def dense_kernel(
    groups, members, cols_ref, outs_ref, tiles_ref, out_ref,
    sbuf, rbuf, mbuf, send_sem, recv_sem, mirror_send, mirror_recv,
):
    part = members // 2
    n = groups * part
    rows, per_row, side, _ = tiles_ref.shape
    grp, row = lax.axis_index("grp"), lax.axis_index("row")
    half, spot = row // part, lax.rem(row, part)
    me = grp * part + spot
    base = (grp * members + row) * rows
    mirror_row = (1 - half) * part + spot
    mirror = {"grp": grp, "row": mirror_row}
    mirror_base = (grp * members + mirror_row) * rows

    def place(s):
        u = lax.rem(me + s, n)
        return u // part, half * part + lax.rem(u, part)

    def target(s):
        g, r = place(s)
        return {"grp": g, "row": r}

    barrier = pltpu.get_barrier_semaphore()
    pl.semaphore_signal(barrier, inc=1, device_id=mirror, device_id_type=MESH)

    def greet(s, carry):
        pl.semaphore_signal(barrier, inc=1, device_id=target(s), device_id_type=MESH)
        return carry

    lax.fori_loop(1, n, greet, 0)

    def asked(s, start):
        g, r = place(s)
        first = (g * members + r) * rows
        t = jnp.int32(0)
        for i in range(rows):
            for k in range(per_row):
                c = cols_ref[k, first + i] - start
                t = jnp.where((c >= 0) & (c < rows), c, t)
        return t

    def copy(s, level):
        return pltpu.make_async_remote_copy(
            src_ref=sbuf.at[level * n + s],
            dst_ref=rbuf.at[level * n + s],
            send_sem=send_sem.at[level * n + s],
            recv_sem=recv_sem.at[level * n + s],
            device_id=target(s),
            device_id_type=MESH,
        )

    def pack(s, carry):
        sbuf[s] = tiles_ref[asked(s, base)]
        return carry

    lax.fori_loop(1, n, pack, 0)
    pl.semaphore_wait(barrier, n)
    across = pltpu.make_async_remote_copy(
        src_ref=tiles_ref,
        dst_ref=mbuf,
        send_sem=mirror_send,
        recv_sem=mirror_recv,
        device_id=mirror,
        device_id_type=MESH,
    )
    across.start()

    def send(s, carry):
        copy(s, 0).start()
        return carry

    lax.fori_loop(1, n, send, 0)
    rbuf[0] = tiles_ref[asked(0, base)]
    across.wait()

    def relay(s, carry):
        sbuf[n + s] = mbuf[asked(s, mirror_base)]
        return carry

    lax.fori_loop(1, n, relay, 0)

    def forward(s, carry):
        copy(s, 1).start()
        return carry

    lax.fori_loop(1, n, forward, 0)
    rbuf[n] = mbuf[asked(0, mirror_base)]

    def land(s, carry):
        copy(s, 0).wait()
        copy(s, 1).wait()
        return carry

    lax.fori_loop(1, n, land, 0)

    def find(owner):
        owner_row = lax.rem(owner, members)
        spot_of = owner // members * part + lax.rem(owner_row, part)
        return lax.rem(me - spot_of + n, n) + jnp.where(owner_row // part == half, 0, n)

    multiply(base, find, cols_ref, outs_ref, tiles_ref, rbuf, out_ref)


def same(lane, rows, groups, members):
    device = lane // rows
    inner = lax.rem(device, members)
    spot = lax.rem(inner, PLANE)
    return device // members, inner // PLANE, spot // 2, lax.rem(spot, 2)


def ones(mask):
    return jnp.where(mask, 1.0, 0.0)


def across(a, b):
    dims = (((1,), (1,)), ((), ()))
    return lax.dot_general(
        a.astype(jnp.bfloat16), b.astype(jnp.bfloat16), dims, preferred_element_type=jnp.float32
    )


def iota(shape, axis):
    return lax.broadcasted_iota(jnp.int32, shape, axis)


def steps(value, bounds):
    return sum((value >= b).astype(jnp.int32) for b in bounds)


def named_rows(cols, here, rows, groups, members):
    g, z, y, x = here
    lines = members // PLANE
    crowd = groups * PLANE
    total = cols.shape[1]
    devices = groups * members
    count = devices + 8
    query = iota((count, total), 0)
    lane = iota((count, total), 1)
    og, oz, oy, ox = same(lane, rows, groups, members)
    rel = PLANE * lax.rem(og + g, 2) + 2 * lax.rem(oy + y, 2) + lax.rem(ox + x, 2)
    up = lax.rem(oz - z + lines, lines)
    alone = (query < devices) & (up == query // crowd) & (rel == lax.rem(query, crowd))
    plane = up == query - devices
    group = ones(alone | plane)
    index = iota((total, total), 0)
    hits = jnp.zeros((count, total), jnp.float32)
    for k in range(cols.shape[0]):
        hits = hits + across(group, ones(index == cols[k : k + 1]))
    return ones(hits > 0.5)


def ranked(stack, cols, upper):
    masks, ranks = [], []
    before = jnp.zeros((stack.shape[0], 1), jnp.float32)
    for j in range(cols.shape[0]):
        m = stack * ones(cols[j : j + 1] >= 0)
        ranks.append(across(m, upper) + before)
        masks.append(m)
        before = before + jnp.sum(m, axis=1, keepdims=True)
    return masks, ranks, before


def slots(held, first, stride, bounds):
    masks, ranks, sums = held
    start = jnp.zeros((8, 1), jnp.float32)
    used, at = [0.0 for _ in masks], [0.0 for _ in masks]
    for k, bound in enumerate(bounds):
        b = 8 * (first + k * stride)
        start = jnp.maximum(start, float(bound))
        for j in range(len(masks)):
            m = masks[j][b : b + 8]
            used[j] = used[j] + m
            at[j] = at[j] + m * (start + ranks[j][b : b + 8])
        start = start + sums[b : b + 8]
    return used, at, start


def triangle(total):
    return ones(iota((total, total), 0) > iota((total, total), 1))


def tables(cols, named, here, rows, groups, members):
    g, z, y, x = here
    lines = members // PLANE
    crowd = groups * PLANE
    devices = groups * members
    total = cols.shape[1]
    per = cols.shape[0]
    lane = iota((8, total), 1)
    sub = iota((8, total), 0)
    og, oz, oy, ox = same(lane, rows, groups, members)
    rel = PLANE * lax.rem(og + g, 2) + 2 * lax.rem(oy + y, 2) + lax.rem(ox + x, 2)
    item = lax.rem(lane, rows)
    lev = steps(item, ROW_CUT)
    local = oz == z
    back = lax.rem(z - oz + lines, lines)
    planes = named[devices : devices + 8]
    mine = jnp.broadcast_to(planes[0:1], (8, total))
    near = named[:crowd]
    upper = triangle(total)
    classes = range(len(ROW_CUT) + 1)
    sends = [planes * ones(local & (lev == k)) for k in classes]
    takes = [mine * ones((back == sub) & (lev == k)) for k in classes]
    held = ranked(jnp.concatenate(sends + takes, axis=0), cols, upper)
    firsts = CUT_B[: len(classes)]
    send_used, send_at, _ = slots(held, 0, 1, firsts)
    take_used, take_at, _ = slots(held, len(classes), 1, firsts)
    arena = crowd * rows * per
    cap_b, cap_c = CUT_B[-1], CUT_C[-1]
    home = [(rel * (rows * per) + item * per + j).astype(jnp.float32) for j in range(per)]
    offset = (arena + (sub - 1) * cap_b).astype(jnp.float32)
    arrived, mids = [], [[] for _ in CUT_C[:-1]]
    for j in range(per):
        spot = jnp.sum(take_used[j] * take_at[j], axis=0, keepdims=True)
        far = jnp.sum(take_used[j] * (offset + take_at[j]), axis=0, keepdims=True)
        arrived.append(jnp.where(local, home[j], jnp.broadcast_to(far, (8, total))))
        part = jnp.where(local, 0, 1 + steps(jnp.broadcast_to(spot, (8, total)), PART_B))
        for c in range(len(mids)):
            mids[c].append(near * ones(part == c))

    def stacked(j):
        return jnp.concatenate([m[j] for m in mids], axis=0)

    masks, ranks = [], []
    before = jnp.zeros((8 * len(mids), 1), jnp.float32)
    for j in range(per):
        m = stacked(j) * ones(cols[j : j + 1] >= 0)
        ranks.append(across(m, upper) + before)
        masks.append(m)
        before = before + jnp.sum(m, axis=1, keepdims=True)
    mid_used, mid_at, _ = slots((masks, ranks, before), 0, 1, CUT_C[:-1])

    def sources(used, at, address, count):
        out = jnp.zeros((8, SPAN * count), jnp.float32)
        slot = iota((SPAN, total), 0)
        for j in range(per):
            spot = jnp.where(used[j] > 0.5, at[j], -1.0).astype(jnp.int32)
            hot = jnp.concatenate([ones(slot == spot[q : q + 1]) for q in range(count)], axis=0)
            out = out + across(address[j], hot)
        return jnp.clip(out.astype(jnp.int32), 0, arena + (lines - 1) * cap_b - 1)

    b_list = sources(send_used, send_at, home, lines)
    c_list = sources(mid_used, mid_at, arrived, crowd)
    final = [jnp.clip(mid_at[j][0:1].astype(jnp.int32), 0, cap_c - 1) for j in range(per)]
    lines_out = []
    for block in [b_list[0:1], c_list[0:1]] + final:
        width = block.shape[1]
        if width % 128:
            block = jnp.concatenate([block, jnp.zeros((1, -width % 128), jnp.int32)], axis=1)
        for h in range(-(-width // 128)):
            lines_out.append(block[:, 128 * h : 128 * h + 128])
    lines_out.append(jnp.zeros((TABLE - len(lines_out), 128), jnp.int32))
    return jnp.concatenate(lines_out, axis=0)


def overflow(cols, named, here, rows, groups, members):
    g, z, y, x = here
    lines = members // PLANE
    crowd = groups * PLANE
    devices = groups * members
    total = cols.shape[1]
    per = cols.shape[0]
    lane = iota((8, total), 1)
    oz = lax.rem(lane // rows, members) // PLANE
    up = lax.rem(oz - z + lines, lines)
    lev = steps(lax.rem(lane, rows), ROW_CUT)
    planes = named[devices : devices + 8]
    classes = range(len(ROW_CUT) + 1)
    stack = [planes * ones((up == s) & (lev == k)) for k in classes for s in range(lines)]
    held = ranked(jnp.concatenate(stack, axis=0), cols, triangle(total))
    sub = iota((8, 1), 0)
    worst = jnp.zeros((8, 1), jnp.float32)
    at = [0.0 for _ in range(per)]
    for s in range(lines):
        _, spot, end = slots(held, s, lines, CUT_B[: len(classes)])
        worst = jnp.maximum(worst, jnp.where((sub < lines) & (sub != s), end - CUT_B[-1], 0.0))
        for j in range(per):
            at[j] = at[j] + spot[j]
    for q in range(lines):
        near = named[crowd * q : crowd * (q + 1)]
        sums = [jnp.zeros((8, 1), jnp.float32) for _ in CUT_C[:-1]]
        for j in range(per):
            load = near * ones(cols[j : j + 1] >= 0)
            part = jnp.where(up == q, 0, 1 + steps(jnp.broadcast_to(at[j][q : q + 1], (8, total)), PART_B))
            for c in range(len(sums)):
                sums[c] = sums[c] + jnp.sum(load * ones(part == c), axis=1, keepdims=True)
        end = jnp.zeros((8, 1), jnp.float32)
        for bound, n in zip(CUT_C, sums):
            end = jnp.maximum(end, float(bound)) + n
        worst = jnp.maximum(worst, end - CUT_C[-1])
    return jnp.max(worst).astype(jnp.int32)


def compact_kernel(
    groups, members, cols_hbm, outs_hbm, tiles_hbm, out_ref, over_ref,
    cols_ref, outs_ref, cols_vec, tiles, parts, arena, b_send, b_recv, c_send, c_recv,
    tab_vec, tab, load_sem, tab_sem, a_out, a_in, b_out, b_in, c_out, c_in,
):
    rows, per, side, _ = tiles.shape
    lines = members // PLANE
    crowd = groups * PLANE
    piece = side // crowd
    g, row = lax.axis_index("grp"), lax.axis_index("row")
    z, spot = row // PLANE, lax.rem(row, PLANE)
    y, x = spot // 2, lax.rem(spot, 2)
    here = (g, z, y, x)
    base = (g * members + row) * rows
    me = g * PLANE + spot
    cuts_a = (0,) + ROW_CUT + (rows,)
    stages = len(cuts_a) - 1
    cap_b = CUT_B[-1]
    chunks_b, chunks_c = len(CUT_B) - 1, len(CUT_C) - 1

    def near_device(u):
        dg, dy, dx = u // PLANE, u // 2 % 2, u % 2
        ns = 2 * lax.rem(y + dy, 2) + lax.rem(x + dx, 2)
        return {"grp": lax.rem(g + dg, 2), "row": z * PLANE + ns}

    def line_device(dz):
        return {"grp": g, "row": lax.rem(z + dz, lines) * PLANE + spot}

    barrier = pltpu.get_barrier_semaphore()
    for dz in range(1, lines):
        pl.semaphore_signal(barrier, inc=1, device_id=line_device(dz), device_id_type=MESH)
    for u in range(crowd - 1, 0, -1):
        pl.semaphore_signal(barrier, inc=1, device_id=near_device(u), device_id_type=MESH)
    loads = [
        pltpu.make_async_copy(cols_hbm, cols_vec, load_sem.at[0]),
        pltpu.make_async_copy(tiles_hbm, tiles, load_sem.at[1]),
        pltpu.make_async_copy(cols_hbm, cols_ref, load_sem.at[2]),
        pltpu.make_async_copy(outs_hbm, outs_ref, load_sem.at[3]),
    ]
    for load in loads:
        load.start()
    loads[1].wait()
    pl.semaphore_wait(barrier, lines - 1 + crowd - 1)

    def a_copy(u, k):
        there = near_device(u)
        start = pl.multiple_of((there["grp"] * PLANE + lax.rem(there["row"], PLANE)) * piece, piece)
        span = pl.ds(cuts_a[k], cuts_a[k + 1] - cuts_a[k])
        return pltpu.make_async_remote_copy(
            src_ref=tiles.at[span, :, pl.ds(start, piece), :],
            dst_ref=parts.at[u, span],
            send_sem=a_out.at[stages * u + k],
            recv_sem=a_in.at[stages * u + k],
            device_id=there,
            device_id_type=MESH,
        )

    order = [3, 7, 1, 2, 5, 6, 4]
    for k in range(stages):
        for u in order:
            a_copy(u, k).start()

    loads[0].wait()
    cols = cols_vec[...]
    named = named_rows(cols, here, rows, groups, members)
    tab_vec[...] = tables(cols, named, here, rows, groups, members)
    move = pltpu.make_async_copy(tab_vec, tab, tab_sem)
    move.start()
    for load in loads[2:]:
        load.wait()
    mine = pl.multiple_of(me * piece, piece)
    for i in range(rows):
        for j in range(per):
            arena[i * per + j] = tiles[i, j, pl.ds(mine, piece), :]
    move.wait()

    def pick(options):
        value = jnp.int32(options[0])
        for at, option in enumerate(options[1:]):
            value = jnp.where(z == at + 1, option, value)
        return value

    far_first = [pick((3, 2, 2, 1)), pick((2, 1, 3, 2)), pick((1, 3, 1, 3))]

    def b_copy(k, dz):
        span = pl.ds(CUT_B[k], CUT_B[k + 1] - CUT_B[k])
        return pltpu.make_async_remote_copy(
            src_ref=b_send.at[dz - 1, span],
            dst_ref=b_recv.at[dz - 1, span],
            send_sem=b_out.at[chunks_b * (dz - 1) + k],
            recv_sem=b_in.at[chunks_b * (dz - 1) + k],
            device_id=line_device(dz),
            device_id_type=MESH,
        )

    def c_copy(k, u):
        span = pl.ds(CUT_C[k], CUT_C[k + 1] - CUT_C[k])
        return pltpu.make_async_remote_copy(
            src_ref=c_send.at[u, span],
            dst_ref=c_recv.at[u, span],
            send_sem=c_out.at[chunks_c * u + k],
            recv_sem=c_in.at[chunks_c * u + k],
            device_id=near_device(u),
            device_id_type=MESH,
        )

    wide_b, wide_c = -(-lines * SPAN // 128), -(-crowd * SPAN // 128)

    def entry(first, at):
        return tab[first + at // 128, at % 128]

    def push_b(k):
        for dz in range(1, lines):
            for q in range(CUT_B[k], CUT_B[k + 1]):
                b_send[dz - 1, q] = arena[entry(0, SPAN * dz + q)]
        for dz in far_first:
            b_copy(k, dz).start()

    def push_c(k):
        for u in order + [0]:
            for q in range(CUT_C[k], CUT_C[k + 1]):
                tile = arena[entry(wide_b, SPAN * u + q)]
                if u:
                    c_send[u, q] = tile
                else:
                    c_recv[0, q] = tile
        for core in range(groups):
            side_of = PLANE * lax.rem(core - g + groups, groups)
            for at in (3, 1, 2):
                c_copy(k, side_of + at).start()
        c_copy(k, PLANE).start()

    for k in range(stages):
        for u in order:
            a_copy(u, k).wait_recv()
            for i in range(cuts_a[k], cuts_a[k + 1]):
                for j in range(per):
                    arena[(u * rows + i) * per + j] = parts[u, i, j]
        push_b(k)
    for k in range(stages, chunks_b):
        push_b(k)
    push_c(0)
    over_ref[0] = overflow(cols, named, here, rows, groups, members)
    held = crowd * rows * per
    sent = 1
    for k in range(chunks_b):
        for dz in range(1, lines):
            b_copy(k, dz).wait_recv()
            for q in range(CUT_B[k], CUT_B[k + 1]):
                arena[held + (dz - 1) * cap_b + q] = b_recv[dz - 1, q]
        if CUT_B[k + 1] in PART_B or k == chunks_b - 1:
            push_c(sent)
            sent += 1

    sources = []
    for piece_of in range(crowd):
        pg, ps = piece_of // PLANE, piece_of % PLANE
        dy, dx = lax.rem(ps // 2 + y, 2), lax.rem(ps % 2 + x, 2)
        sources.append(PLANE * lax.rem(pg + g, 2) + 2 * dy + dx)
    for k in range(chunks_c):
        for u in order:
            c_copy(k, u).wait_recv()

    outs_row = outs_ref.shape[0]
    wide = cols_ref.shape[1] // 128
    for i in range(rows):
        left = jnp.concatenate([tiles[i, k] for k in range(per)], axis=1)
        stack = []
        for k in range(per):
            c = cols_ref[k, base + i]
            safe = jnp.maximum(c, 0)
            line = []
            for p in range(outs_row):
                o = outs_ref[p, i]
                which = jnp.int32(0)
                hit = jnp.int32(0)
                for j in range(per):
                    match = cols_ref[j, safe] == o
                    which = jnp.where(match, j, which)
                    hit = jnp.where(match & (c >= 0), 1, hit)
                slot = tab[wide_b + wide_c + wide * which + safe // 128, lax.rem(safe, 128)]
                tile = jnp.concatenate([c_recv[s, slot] for s in sources], axis=0)
                line.append(tile * hit.astype(jnp.float32).astype(jnp.bfloat16))
            stack.append(jnp.concatenate(line, axis=1))
        right = jnp.concatenate(stack, axis=0)
        prod = jnp.dot(left, right, preferred_element_type=jnp.float32).astype(jnp.bfloat16)
        for p in range(outs_row):
            out_ref[i, p] = prod[:, p * side : (p + 1) * side]

    for u in order:
        for k in range(stages):
            a_copy(u, k).wait_send()
        for k in range(chunks_c):
            c_copy(k, u).wait_send()
    for dz in range(1, lines):
        for k in range(chunks_b):
            b_copy(k, dz).wait_send()


def params(identity):
    return pltpu.CompilerParams(
        collective_id=identity, has_side_effects=True, vmem_limit_bytes=56 * 1024 * 1024
    )


def shards(block_tiles, tile_columns, requests, output_columns):
    groups = lax.axis_size("grp")
    members = lax.axis_size("row")
    n = groups * members
    rows, per_row, side, _ = block_tiles.shape
    vmem = pl.BlockSpec(memory_space=pltpu.VMEM)
    smem = pl.BlockSpec(memory_space=pltpu.SMEM)
    out = jax.ShapeDtypeStruct((rows, output_columns.shape[1], side, side), jnp.bfloat16)
    tile_rows = lambda count: pltpu.VMEM((count, per_row, side, side), jnp.bfloat16)
    columns, outs = tile_columns.T, output_columns.T

    def dense():
        return pl.pallas_call(
            functools.partial(dense_kernel, groups, members),
            out_shape=out,
            in_specs=[smem, smem, vmem],
            out_specs=vmem,
            scratch_shapes=[
                tile_rows(n),
                tile_rows(n),
                tile_rows(rows),
                pltpu.SemaphoreType.DMA((n,)),
                pltpu.SemaphoreType.DMA((n,)),
                pltpu.SemaphoreType.DMA,
                pltpu.SemaphoreType.DMA,
            ],
            compiler_params=params(0),
        )(columns, outs, block_tiles)

    lines = members // PLANE
    crowd = groups * PLANE
    cap_b, cap_c = CUT_B[-1], CUT_C[-1]
    held = crowd * rows * per_row + (lines - 1) * cap_b
    fits = groups == 2 and members == 4 * PLANE and per_row == 2 and rows > ROW_CUT[-1]
    fits = fits and tile_columns.shape[0] % 128 == 0 and side % (16 * crowd) == 0 and held <= 256
    if not fits:
        return dense()
    piece = side // crowd
    pieces = lambda *lead: pltpu.VMEM((*lead, piece, side), jnp.bfloat16)
    dma = pltpu.SemaphoreType.DMA
    hbm = pl.BlockSpec(memory_space=pl.ANY)
    stages, chunks_b, chunks_c = len(ROW_CUT) + 1, len(CUT_B) - 1, len(CUT_C) - 1
    compact, over = pl.pallas_call(
        functools.partial(compact_kernel, groups, members),
        out_shape=(out, jax.ShapeDtypeStruct((1,), jnp.int32)),
        in_specs=[hbm, hbm, hbm],
        out_specs=(vmem, smem),
        scratch_shapes=[
            pltpu.SMEM(columns.shape, jnp.int32),
            pltpu.SMEM(outs.shape, jnp.int32),
            pltpu.VMEM(columns.shape, jnp.int32),
            pltpu.VMEM(block_tiles.shape, jnp.bfloat16),
            pieces(crowd, rows, per_row),
            pieces(held),
            pieces(lines - 1, cap_b),
            pieces(lines - 1, cap_b),
            pieces(crowd, cap_c),
            pieces(crowd, cap_c),
            pltpu.VMEM((TABLE, 128), jnp.int32),
            pltpu.SMEM((TABLE, 128), jnp.int32),
            dma((4,)),
            dma,
            dma((stages * crowd,)),
            dma((stages * crowd,)),
            dma((chunks_b * (lines - 1),)),
            dma((chunks_b * (lines - 1),)),
            dma((chunks_c * crowd,)),
            dma((chunks_c * crowd,)),
        ],
        compiler_params=params(1),
    )(columns, outs, block_tiles)
    return lax.cond(over[0] > 0, dense, lambda: compact)


def solution(mesh):
    placed = (
        P(("grp", "row"), None, None, None),
        P(),
        P(("grp", "row"), None),
        P(("grp", "row"), None),
    )
    return jax.shard_map(
        shards,
        mesh=mesh,
        in_specs=placed,
        out_specs=P(("grp", "row"), None, None, None),
        check_vma=False,
    )
```

```python
import functools

import jax
import jax.numpy as jnp
from jax import lax
from jax.experimental import pallas as pl
from jax.experimental.pallas import tpu as pltpu
from jax.sharding import PartitionSpec as P

MESH = pl.DeviceIdType.MESH
PLANE = 4
CUT_A = (0, 2, 6, 12)
START_B = (0, 6, 20)
CUT_B = (0, 6, 13, 20, 32)
CLASS_B = (0, 1, 1, 2)
PART_B = (13, 20)
CUT_C = (0, 3, 10, 16, 21)
SPAN = 40
TABLE = 16


def multiply(base, find, cols_ref, outs_ref, tiles_ref, rbuf, out_ref):
    rows, per_row, side, _ = tiles_ref.shape
    outs_row = outs_ref.shape[0]
    for i in range(rows):
        left = jnp.concatenate([tiles_ref[i, k] for k in range(per_row)], axis=1)
        stack = []
        for k in range(per_row):
            c = cols_ref[k, base + i]
            safe = jnp.maximum(c, 0)
            slot = find(safe // rows)
            line = []
            for p in range(outs_row):
                o = outs_ref[p, i]
                which = jnp.int32(0)
                hit = jnp.int32(0)
                for j in range(per_row):
                    same = cols_ref[j, safe] == o
                    which = jnp.where(same, j, which)
                    hit = jnp.where(same & (c >= 0), 1, hit)
                tile = rbuf[slot, which]
                line.append(tile * hit.astype(jnp.float32).astype(jnp.bfloat16))
            stack.append(jnp.concatenate(line, axis=1))
        right = jnp.concatenate(stack, axis=0)
        prod = jnp.dot(left, right, preferred_element_type=jnp.float32).astype(jnp.bfloat16)
        for p in range(outs_row):
            out_ref[i, p] = prod[:, p * side : (p + 1) * side]


def dense_kernel(
    groups, members, cols_ref, outs_ref, tiles_ref, out_ref,
    sbuf, rbuf, mbuf, send_sem, recv_sem, mirror_send, mirror_recv,
):
    part = members // 2
    n = groups * part
    rows, per_row, side, _ = tiles_ref.shape
    grp, row = lax.axis_index("grp"), lax.axis_index("row")
    half, spot = row // part, lax.rem(row, part)
    me = grp * part + spot
    base = (grp * members + row) * rows
    mirror_row = (1 - half) * part + spot
    mirror = {"grp": grp, "row": mirror_row}
    mirror_base = (grp * members + mirror_row) * rows

    def place(s):
        u = lax.rem(me + s, n)
        return u // part, half * part + lax.rem(u, part)

    def target(s):
        g, r = place(s)
        return {"grp": g, "row": r}

    barrier = pltpu.get_barrier_semaphore()
    pl.semaphore_signal(barrier, inc=1, device_id=mirror, device_id_type=MESH)

    def greet(s, carry):
        pl.semaphore_signal(barrier, inc=1, device_id=target(s), device_id_type=MESH)
        return carry

    lax.fori_loop(1, n, greet, 0)

    def asked(s, start):
        g, r = place(s)
        first = (g * members + r) * rows
        t = jnp.int32(0)
        for i in range(rows):
            for k in range(per_row):
                c = cols_ref[k, first + i] - start
                t = jnp.where((c >= 0) & (c < rows), c, t)
        return t

    def copy(s, level):
        return pltpu.make_async_remote_copy(
            src_ref=sbuf.at[level * n + s],
            dst_ref=rbuf.at[level * n + s],
            send_sem=send_sem.at[level * n + s],
            recv_sem=recv_sem.at[level * n + s],
            device_id=target(s),
            device_id_type=MESH,
        )

    def pack(s, carry):
        sbuf[s] = tiles_ref[asked(s, base)]
        return carry

    lax.fori_loop(1, n, pack, 0)
    pl.semaphore_wait(barrier, n)
    across = pltpu.make_async_remote_copy(
        src_ref=tiles_ref,
        dst_ref=mbuf,
        send_sem=mirror_send,
        recv_sem=mirror_recv,
        device_id=mirror,
        device_id_type=MESH,
    )
    across.start()

    def send(s, carry):
        copy(s, 0).start()
        return carry

    lax.fori_loop(1, n, send, 0)
    rbuf[0] = tiles_ref[asked(0, base)]
    across.wait()

    def relay(s, carry):
        sbuf[n + s] = mbuf[asked(s, mirror_base)]
        return carry

    lax.fori_loop(1, n, relay, 0)

    def forward(s, carry):
        copy(s, 1).start()
        return carry

    lax.fori_loop(1, n, forward, 0)
    rbuf[n] = mbuf[asked(0, mirror_base)]

    def land(s, carry):
        copy(s, 0).wait()
        copy(s, 1).wait()
        return carry

    lax.fori_loop(1, n, land, 0)

    def find(owner):
        owner_row = lax.rem(owner, members)
        spot_of = owner // members * part + lax.rem(owner_row, part)
        return lax.rem(me - spot_of + n, n) + jnp.where(owner_row // part == half, 0, n)

    multiply(base, find, cols_ref, outs_ref, tiles_ref, rbuf, out_ref)


def same(lane, rows, groups, members):
    device = lane // rows
    inner = lax.rem(device, members)
    spot = lax.rem(inner, PLANE)
    return device // members, inner // PLANE, spot // 2, lax.rem(spot, 2)


def ones(mask):
    return jnp.where(mask, 1.0, 0.0)


def across(a, b):
    dims = (((1,), (1,)), ((), ()))
    return lax.dot_general(
        a.astype(jnp.bfloat16), b.astype(jnp.bfloat16), dims, preferred_element_type=jnp.float32
    )


def iota(shape, axis):
    return lax.broadcasted_iota(jnp.int32, shape, axis)


def steps(value, bounds):
    return sum((value >= b).astype(jnp.int32) for b in bounds)


def named_rows(cols, here, rows, groups, members):
    g, z, y, x = here
    lines = members // PLANE
    crowd = groups * PLANE
    total = cols.shape[1]
    devices = groups * members
    count = devices + 8
    query = iota((count, total), 0)
    lane = iota((count, total), 1)
    og, oz, oy, ox = same(lane, rows, groups, members)
    rel = PLANE * lax.rem(og + g, 2) + 2 * lax.rem(oy + y, 2) + lax.rem(ox + x, 2)
    up = lax.rem(oz - z + lines, lines)
    alone = (query < devices) & (up == query // crowd) & (rel == lax.rem(query, crowd))
    plane = up == query - devices
    group = ones(alone | plane)
    index = iota((total, total), 0)
    hits = jnp.zeros((count, total), jnp.float32)
    for k in range(cols.shape[0]):
        hits = hits + across(group, ones(index == cols[k : k + 1]))
    return ones(hits > 0.5)


def ranked(masks, upper):
    ranks = []
    before = jnp.zeros((masks[0].shape[0], 1), jnp.float32)
    for m in masks:
        ranks.append(across(m, upper) + before)
        before = before + jnp.sum(m, axis=1, keepdims=True)
    return masks, ranks, before


def slots(held, first, stride, bounds):
    masks, ranks, sums = held
    start = jnp.zeros((8, 1), jnp.float32)
    used, at = [0.0 for _ in masks], [0.0 for _ in masks]
    for k, bound in enumerate(bounds):
        b = 8 * (first + k * stride)
        start = jnp.maximum(start, float(bound))
        for j in range(len(masks)):
            m = masks[j][b : b + 8]
            used[j] = used[j] + m
            at[j] = at[j] + m * (start + ranks[j][b : b + 8])
        start = start + sums[b : b + 8]
    return used, at, start


def triangle(total):
    return ones(iota((total, total), 0) > iota((total, total), 1))


def column(slot, spot, count):
    hot = [ones(slot == spot[q : q + 1]) for q in range(count)]
    return jnp.concatenate(hot, axis=0)


def owned(cols, named, here, rows, groups, members):
    devices = groups * members
    total = cols.shape[1]
    per = cols.shape[0]
    wanted = ones(jnp.sum(named[devices : devices + 8], axis=0, keepdims=True) > 0.5)
    masks = [jnp.broadcast_to(wanted * ones(cols[j : j + 1] >= 0), (8, total)) for j in range(per)]
    a, b = iota((total, total), 0), iota((total, total), 1)
    block = a // rows == b // rows
    upper, whole = ones(block & (a > b)), ones(block)
    ranks = []
    before = jnp.zeros((8, total), jnp.float32)
    for m in masks:
        ranks.append(across(m, upper) + before)
        before = before + across(m, whole)
    lane = iota((8, total), 1)
    og, oz, oy, ox = same(lane, rows, groups, members)
    g, z, y, x = here
    mine = (og == g) & (oz == z) & (oy == y) & (ox == x)
    item = lax.rem(lane, rows)
    picks = jnp.zeros((8, 128), jnp.float32)
    slot = iota((128, total), 0)
    for j in range(per):
        spot = jnp.where(mine & (masks[j] > 0.5), ranks[j], -1.0).astype(jnp.int32)
        picks = picks + across((item * per + j).astype(jnp.float32), column(slot, spot, 1))
    picks = jnp.clip(picks.astype(jnp.int32), 0, rows * per - 1)
    return ranks, before, picks


def tables(cols, named, ranks_a, here, rows, groups, members):
    g, z, y, x = here
    lines = members // PLANE
    crowd = groups * PLANE
    devices = groups * members
    total = cols.shape[1]
    per = cols.shape[0]
    lane = iota((8, total), 1)
    sub = iota((8, total), 0)
    og, oz, oy, ox = same(lane, rows, groups, members)
    rel = PLANE * lax.rem(og + g, 2) + 2 * lax.rem(oy + y, 2) + lax.rem(ox + x, 2)
    local = oz == z
    back = lax.rem(z - oz + lines, lines)
    planes = named[devices : devices + 8]
    mine = jnp.broadcast_to(planes[0:1], (8, total))
    near = named[:crowd]
    upper = triangle(total)
    classes = range(len(START_B))
    present = [ones(cols[j : j + 1] >= 0) for j in range(per)]
    sends, takes = planes * ones(local), mine * ones(back == sub)
    stacks = []
    for j in range(per):
        lev = steps(ranks_a[j], CUT_A[1:-1])
        kept = [present[j] * ones(lev == k) for k in classes]
        stacks.append(jnp.concatenate([sends * m for m in kept] + [takes * m for m in kept], axis=0))
    held = ranked(stacks, upper)
    send_used, send_at, _ = slots(held, 0, 1, START_B)
    take_used, take_at, _ = slots(held, len(classes), 1, START_B)
    cap_a, cap_b, cap_c = CUT_A[-1], CUT_B[-1], CUT_C[-1]
    arena = crowd * cap_a
    first = (rel * cap_a).astype(jnp.float32)
    home = [first + jnp.minimum(ranks_a[j], cap_a - 1.0) for j in range(per)]
    offset = (arena + (sub - 1) * cap_b).astype(jnp.float32)
    arrived, mids = [], []
    for j in range(per):
        spot = jnp.sum(take_used[j] * take_at[j], axis=0, keepdims=True)
        far = jnp.sum(take_used[j] * (offset + take_at[j]), axis=0, keepdims=True)
        arrived.append(jnp.where(local, home[j], jnp.broadcast_to(far, (8, total))))
        part = jnp.where(local, 0, 1 + steps(jnp.broadcast_to(spot, (8, total)), PART_B))
        kept = near * present[j]
        mids.append(jnp.concatenate([kept * ones(part == c) for c in range(len(CUT_C) - 1)], axis=0))
    mid_used, mid_at, _ = slots(ranked(mids, upper), 0, 1, CUT_C[:-1])

    def sources(used, at, address, count):
        out = jnp.zeros((8, SPAN * count), jnp.float32)
        slot = iota((SPAN, total), 0)
        for j in range(per):
            spot = jnp.where(used[j] > 0.5, at[j], -1.0).astype(jnp.int32)
            out = out + across(address[j], column(slot, spot, count))
        return jnp.clip(out.astype(jnp.int32), 0, arena + (lines - 1) * cap_b - 1)

    b_list = sources(send_used, send_at, home, lines)
    c_list = sources(mid_used, mid_at, arrived, crowd)
    final = [jnp.clip(mid_at[j][0:1].astype(jnp.int32), 0, cap_c - 1) for j in range(per)]
    lines_out = []
    for block in [b_list[0:1], c_list[0:1]] + final:
        width = block.shape[1]
        if width % 128:
            block = jnp.concatenate([block, jnp.zeros((1, -width % 128), jnp.int32)], axis=1)
        for h in range(-(-width // 128)):
            lines_out.append(block[:, 128 * h : 128 * h + 128])
    lines_out.append(jnp.zeros((TABLE - len(lines_out), 128), jnp.int32))
    return jnp.concatenate(lines_out, axis=0)


def overflow(cols, named, ranks_a, loads_a, here, rows, groups, members):
    g, z, y, x = here
    lines = members // PLANE
    crowd = groups * PLANE
    devices = groups * members
    total = cols.shape[1]
    per = cols.shape[0]
    lane = iota((8, total), 1)
    oz = lax.rem(lane // rows, members) // PLANE
    up = lax.rem(oz - z + lines, lines)
    planes = named[devices : devices + 8]
    classes = range(len(START_B))
    present = [ones(cols[j : j + 1] >= 0) for j in range(per)]
    stacks = []
    for j in range(per):
        lev = steps(ranks_a[j], CUT_A[1:-1])
        kept = planes * present[j]
        stacks.append(
            jnp.concatenate(
                [kept * ones((up == s) & (lev == k)) for k in classes for s in range(lines)], axis=0
            )
        )
    held = ranked(stacks, triangle(total))
    sub = iota((8, 1), 0)
    worst = jnp.maximum(jnp.max(loads_a, axis=1, keepdims=True) - CUT_A[-1], 0.0)
    at = [0.0 for _ in range(per)]
    for s in range(lines):
        _, spot, end = slots(held, s, lines, START_B)
        worst = jnp.maximum(worst, jnp.where((sub < lines) & (sub != s), end - CUT_B[-1], 0.0))
        for j in range(per):
            at[j] = at[j] + spot[j]
    for q in range(lines):
        near = named[crowd * q : crowd * (q + 1)]
        sums = [jnp.zeros((8, 1), jnp.float32) for _ in CUT_C[:-1]]
        for j in range(per):
            load = near * present[j]
            spot = jnp.broadcast_to(at[j][q : q + 1], (8, total))
            part = jnp.where(up == q, 0, 1 + steps(spot, PART_B))
            for c in range(len(sums)):
                sums[c] = sums[c] + jnp.sum(load * ones(part == c), axis=1, keepdims=True)
        end = jnp.zeros((8, 1), jnp.float32)
        for bound, n in zip(CUT_C, sums):
            end = jnp.maximum(end, float(bound)) + n
        worst = jnp.maximum(worst, end - CUT_C[-1])
    return jnp.max(worst).astype(jnp.int32)


def compact_kernel(
    groups, members, cols_hbm, outs_hbm, tiles_hbm, out_ref, over_ref,
    cols_ref, outs_ref, cols_vec, tiles, a_send, parts, arena, b_send, b_recv, c_send, c_recv,
    own_vec, own, tab_vec, tab, load_sem, tab_sem, a_out, a_in, b_out, b_in, c_out, c_in,
):
    rows, per, side, _ = tiles.shape
    lines = members // PLANE
    crowd = groups * PLANE
    piece = side // crowd
    g, row = lax.axis_index("grp"), lax.axis_index("row")
    z, spot = row // PLANE, lax.rem(row, PLANE)
    y, x = spot // 2, lax.rem(spot, 2)
    here = (g, z, y, x)
    base = (g * members + row) * rows
    me = g * PLANE + spot
    stages, cap_a, cap_b = len(CUT_A) - 1, CUT_A[-1], CUT_B[-1]
    chunks_b, chunks_c = len(CUT_B) - 1, len(CUT_C) - 1

    def near_device(u):
        dg, dy, dx = u // PLANE, u // 2 % 2, u % 2
        ns = 2 * lax.rem(y + dy, 2) + lax.rem(x + dx, 2)
        return {"grp": lax.rem(g + dg, 2), "row": z * PLANE + ns}

    def line_device(dz):
        return {"grp": g, "row": lax.rem(z + dz, lines) * PLANE + spot}

    barrier = pltpu.get_barrier_semaphore()
    for dz in range(1, lines):
        pl.semaphore_signal(barrier, inc=1, device_id=line_device(dz), device_id_type=MESH)
    for u in range(crowd - 1, 0, -1):
        pl.semaphore_signal(barrier, inc=1, device_id=near_device(u), device_id_type=MESH)
    loads = [
        pltpu.make_async_copy(cols_hbm, cols_vec, load_sem.at[0]),
        pltpu.make_async_copy(tiles_hbm, tiles, load_sem.at[1]),
        pltpu.make_async_copy(cols_hbm, cols_ref, load_sem.at[2]),
        pltpu.make_async_copy(outs_hbm, outs_ref, load_sem.at[3]),
    ]
    for load in loads:
        load.start()
    loads[0].wait()
    cols = cols_vec[...]
    named = named_rows(cols, here, rows, groups, members)
    ranks_a, loads_a, picks = owned(cols, named, here, rows, groups, members)
    own_vec[...] = picks
    move = pltpu.make_async_copy(own_vec, own, tab_sem.at[0])
    move.start()
    for load in loads[1:]:
        load.wait()
    move.wait()
    for q in range(cap_a):
        pick = own[0, q]
        a_send[q] = tiles[pick // per, lax.rem(pick, per)]
    pl.semaphore_wait(barrier, lines - 1 + crowd - 1)

    def a_copy(u, k):
        there = near_device(u)
        start = pl.multiple_of((there["grp"] * PLANE + lax.rem(there["row"], PLANE)) * piece, piece)
        span = pl.ds(CUT_A[k], CUT_A[k + 1] - CUT_A[k])
        return pltpu.make_async_remote_copy(
            src_ref=a_send.at[span, pl.ds(start, piece), :],
            dst_ref=parts.at[u, span],
            send_sem=a_out.at[stages * u + k],
            recv_sem=a_in.at[stages * u + k],
            device_id=there,
            device_id_type=MESH,
        )

    order = [3, 7, 1, 2, 5, 6, 4]
    for k in range(stages):
        for u in order:
            a_copy(u, k).start()

    tab_vec[...] = tables(cols, named, ranks_a, here, rows, groups, members)
    move = pltpu.make_async_copy(tab_vec, tab, tab_sem.at[1])
    move.start()
    mine = pl.multiple_of(me * piece, piece)
    for q in range(cap_a):
        arena[q] = a_send[q, pl.ds(mine, piece), :]
    move.wait()

    def pick(options):
        value = jnp.int32(options[0])
        for at, option in enumerate(options[1:]):
            value = jnp.where(z == at + 1, option, value)
        return value

    far_first = [pick((3, 2, 2, 1)), pick((2, 1, 3, 2)), pick((1, 3, 1, 3))]

    def b_copy(k, dz):
        span = pl.ds(CUT_B[k], CUT_B[k + 1] - CUT_B[k])
        return pltpu.make_async_remote_copy(
            src_ref=b_send.at[dz - 1, span],
            dst_ref=b_recv.at[dz - 1, span],
            send_sem=b_out.at[chunks_b * (dz - 1) + k],
            recv_sem=b_in.at[chunks_b * (dz - 1) + k],
            device_id=line_device(dz),
            device_id_type=MESH,
        )

    def c_copy(k, u):
        span = pl.ds(CUT_C[k], CUT_C[k + 1] - CUT_C[k])
        return pltpu.make_async_remote_copy(
            src_ref=c_send.at[u, span],
            dst_ref=c_recv.at[u, span],
            send_sem=c_out.at[chunks_c * u + k],
            recv_sem=c_in.at[chunks_c * u + k],
            device_id=near_device(u),
            device_id_type=MESH,
        )

    wide_b, wide_c = -(-lines * SPAN // 128), -(-crowd * SPAN // 128)

    def entry(first, at):
        return tab[first + at // 128, at % 128]

    def push_b(k):
        for dz in range(1, lines):
            for q in range(CUT_B[k], CUT_B[k + 1]):
                b_send[dz - 1, q] = arena[entry(0, SPAN * dz + q)]
        for dz in far_first:
            b_copy(k, dz).start()

    def push_c(k):
        for u in order + [0]:
            for q in range(CUT_C[k], CUT_C[k + 1]):
                tile = arena[entry(wide_b, SPAN * u + q)]
                if u:
                    c_send[u, q] = tile
                else:
                    c_recv[0, q] = tile
        for core in range(groups):
            side_of = PLANE * lax.rem(core - g + groups, groups)
            for at in (3, 1, 2):
                c_copy(k, side_of + at).start()
        c_copy(k, PLANE).start()

    for k in range(stages):
        for u in order:
            a_copy(u, k).wait_recv()
            for q in range(CUT_A[k], CUT_A[k + 1]):
                arena[u * cap_a + q] = parts[u, q]
        for part in range(chunks_b):
            if CLASS_B[part] == k:
                push_b(part)
    push_c(0)
    over_ref[0] = overflow(cols, named, ranks_a, loads_a, here, rows, groups, members)
    held = crowd * cap_a
    sent = 1
    for k in range(chunks_b):
        for dz in range(1, lines):
            b_copy(k, dz).wait_recv()
            for q in range(CUT_B[k], CUT_B[k + 1]):
                arena[held + (dz - 1) * cap_b + q] = b_recv[dz - 1, q]
        if CUT_B[k + 1] in PART_B or k == chunks_b - 1:
            push_c(sent)
            sent += 1

    sources = []
    for piece_of in range(crowd):
        pg, ps = piece_of // PLANE, piece_of % PLANE
        dy, dx = lax.rem(ps // 2 + y, 2), lax.rem(ps % 2 + x, 2)
        sources.append(PLANE * lax.rem(pg + g, 2) + 2 * dy + dx)
    for k in range(chunks_c):
        for u in order:
            c_copy(k, u).wait_recv()

    outs_row = outs_ref.shape[0]
    wide = cols_ref.shape[1] // 128
    for i in range(rows):
        left = jnp.concatenate([tiles[i, k] for k in range(per)], axis=1)
        stack = []
        for k in range(per):
            c = cols_ref[k, base + i]
            safe = jnp.maximum(c, 0)
            line = []
            for p in range(outs_row):
                o = outs_ref[p, i]
                which = jnp.int32(0)
                hit = jnp.int32(0)
                for j in range(per):
                    match = cols_ref[j, safe] == o
                    which = jnp.where(match, j, which)
                    hit = jnp.where(match & (c >= 0), 1, hit)
                slot = tab[wide_b + wide_c + wide * which + safe // 128, lax.rem(safe, 128)]
                tile = jnp.concatenate([c_recv[s, slot] for s in sources], axis=0)
                line.append(tile * hit.astype(jnp.float32).astype(jnp.bfloat16))
            stack.append(jnp.concatenate(line, axis=1))
        right = jnp.concatenate(stack, axis=0)
        prod = jnp.dot(left, right, preferred_element_type=jnp.float32).astype(jnp.bfloat16)
        for p in range(outs_row):
            out_ref[i, p] = prod[:, p * side : (p + 1) * side]

    for u in order:
        for k in range(stages):
            a_copy(u, k).wait_send()
        for k in range(chunks_c):
            c_copy(k, u).wait_send()
    for dz in range(1, lines):
        for k in range(chunks_b):
            b_copy(k, dz).wait_send()


def params(identity):
    return pltpu.CompilerParams(
        collective_id=identity, has_side_effects=True, vmem_limit_bytes=56 * 1024 * 1024
    )


def shards(block_tiles, tile_columns, requests, output_columns):
    groups = lax.axis_size("grp")
    members = lax.axis_size("row")
    n = groups * members
    rows, per_row, side, _ = block_tiles.shape
    vmem = pl.BlockSpec(memory_space=pltpu.VMEM)
    smem = pl.BlockSpec(memory_space=pltpu.SMEM)
    out = jax.ShapeDtypeStruct((rows, output_columns.shape[1], side, side), jnp.bfloat16)
    tile_rows = lambda count: pltpu.VMEM((count, per_row, side, side), jnp.bfloat16)
    columns, outs = tile_columns.T, output_columns.T

    def dense():
        return pl.pallas_call(
            functools.partial(dense_kernel, groups, members),
            out_shape=out,
            in_specs=[smem, smem, vmem],
            out_specs=vmem,
            scratch_shapes=[
                tile_rows(n),
                tile_rows(n),
                tile_rows(rows),
                pltpu.SemaphoreType.DMA((n,)),
                pltpu.SemaphoreType.DMA((n,)),
                pltpu.SemaphoreType.DMA,
                pltpu.SemaphoreType.DMA,
            ],
            compiler_params=params(0),
        )(columns, outs, block_tiles)

    lines = members // PLANE
    crowd = groups * PLANE
    cap_b, cap_c = CUT_B[-1], CUT_C[-1]
    held = crowd * CUT_A[-1] + (lines - 1) * cap_b
    fits = groups == 2 and members == 4 * PLANE and per_row == 2 and CUT_A[-1] <= 128
    fits = fits and tile_columns.shape[0] % 128 == 0 and side % (16 * crowd) == 0 and held <= 256
    if not fits:
        return dense()
    piece = side // crowd
    pieces = lambda *lead: pltpu.VMEM((*lead, piece, side), jnp.bfloat16)
    dma = pltpu.SemaphoreType.DMA
    hbm = pl.BlockSpec(memory_space=pl.ANY)
    stages, chunks_b, chunks_c = len(CUT_A) - 1, len(CUT_B) - 1, len(CUT_C) - 1
    compact, over = pl.pallas_call(
        functools.partial(compact_kernel, groups, members),
        out_shape=(out, jax.ShapeDtypeStruct((1,), jnp.int32)),
        in_specs=[hbm, hbm, hbm],
        out_specs=(vmem, smem),
        scratch_shapes=[
            pltpu.SMEM(columns.shape, jnp.int32),
            pltpu.SMEM(outs.shape, jnp.int32),
            pltpu.VMEM(columns.shape, jnp.int32),
            pltpu.VMEM(block_tiles.shape, jnp.bfloat16),
            pltpu.VMEM((CUT_A[-1], side, side), jnp.bfloat16),
            pieces(crowd, CUT_A[-1]),
            pieces(held),
            pieces(lines - 1, cap_b),
            pieces(lines - 1, cap_b),
            pieces(crowd, cap_c),
            pieces(crowd, cap_c),
            pltpu.VMEM((8, 128), jnp.int32),
            pltpu.SMEM((8, 128), jnp.int32),
            pltpu.VMEM((TABLE, 128), jnp.int32),
            pltpu.SMEM((TABLE, 128), jnp.int32),
            dma((4,)),
            dma((2,)),
            dma((stages * crowd,)),
            dma((stages * crowd,)),
            dma((chunks_b * (lines - 1),)),
            dma((chunks_b * (lines - 1),)),
            dma((chunks_c * crowd,)),
            dma((chunks_c * crowd,)),
        ],
        compiler_params=params(1),
    )(columns, outs, block_tiles)
    return lax.cond(over[0] > 0, dense, lambda: compact)


def solution(mesh):
    placed = (
        P(("grp", "row"), None, None, None),
        P(),
        P(("grp", "row"), None),
        P(("grp", "row"), None),
    )
    return jax.shard_map(
        shards,
        mesh=mesh,
        in_specs=placed,
        out_specs=P(("grp", "row"), None, None, None),
        check_vma=False,
    )
```

```python
import functools

import jax
import jax.numpy as jnp
from jax import lax
from jax.experimental import pallas as pl
from jax.experimental.pallas import tpu as pltpu
from jax.sharding import PartitionSpec as P

MESH = pl.DeviceIdType.MESH
PLANE = 4
CUT_A = (0, 2, 6, 12)
START_B = (0, 6, 20)
CUT_B = (0, 6, 13, 20, 32)
CLASS_B = (0, 1, 1, 2)
PART_B = (13, 20)
CUT_C = (0, 3, 10, 16, 21)
SPAN = 40
TABLE = 16


def multiply(base, find, cols_ref, outs_ref, tiles_ref, rbuf, out_ref):
    rows, per_row, side, _ = tiles_ref.shape
    outs_row = outs_ref.shape[0]
    for i in range(rows):
        left = jnp.concatenate([tiles_ref[i, k] for k in range(per_row)], axis=1)
        stack = []
        for k in range(per_row):
            c = cols_ref[k, base + i]
            safe = jnp.maximum(c, 0)
            slot = find(safe // rows)
            line = []
            for p in range(outs_row):
                o = outs_ref[p, i]
                which = jnp.int32(0)
                hit = jnp.int32(0)
                for j in range(per_row):
                    same = cols_ref[j, safe] == o
                    which = jnp.where(same, j, which)
                    hit = jnp.where(same & (c >= 0), 1, hit)
                tile = rbuf[slot, which]
                line.append(tile * hit.astype(jnp.float32).astype(jnp.bfloat16))
            stack.append(jnp.concatenate(line, axis=1))
        right = jnp.concatenate(stack, axis=0)
        prod = jnp.dot(left, right, preferred_element_type=jnp.float32).astype(jnp.bfloat16)
        for p in range(outs_row):
            out_ref[i, p] = prod[:, p * side : (p + 1) * side]


def dense_kernel(
    groups, members, cols_ref, outs_ref, tiles_ref, out_ref,
    sbuf, rbuf, mbuf, send_sem, recv_sem, mirror_send, mirror_recv,
):
    part = members // 2
    n = groups * part
    rows, per_row, side, _ = tiles_ref.shape
    grp, row = lax.axis_index("grp"), lax.axis_index("row")
    half, spot = row // part, lax.rem(row, part)
    me = grp * part + spot
    base = (grp * members + row) * rows
    mirror_row = (1 - half) * part + spot
    mirror = {"grp": grp, "row": mirror_row}
    mirror_base = (grp * members + mirror_row) * rows

    def place(s):
        u = lax.rem(me + s, n)
        return u // part, half * part + lax.rem(u, part)

    def target(s):
        g, r = place(s)
        return {"grp": g, "row": r}

    barrier = pltpu.get_barrier_semaphore()
    pl.semaphore_signal(barrier, inc=1, device_id=mirror, device_id_type=MESH)

    def greet(s, carry):
        pl.semaphore_signal(barrier, inc=1, device_id=target(s), device_id_type=MESH)
        return carry

    lax.fori_loop(1, n, greet, 0)

    def asked(s, start):
        g, r = place(s)
        first = (g * members + r) * rows
        t = jnp.int32(0)
        for i in range(rows):
            for k in range(per_row):
                c = cols_ref[k, first + i] - start
                t = jnp.where((c >= 0) & (c < rows), c, t)
        return t

    def copy(s, level):
        return pltpu.make_async_remote_copy(
            src_ref=sbuf.at[level * n + s],
            dst_ref=rbuf.at[level * n + s],
            send_sem=send_sem.at[level * n + s],
            recv_sem=recv_sem.at[level * n + s],
            device_id=target(s),
            device_id_type=MESH,
        )

    def pack(s, carry):
        sbuf[s] = tiles_ref[asked(s, base)]
        return carry

    lax.fori_loop(1, n, pack, 0)
    pl.semaphore_wait(barrier, n)
    across = pltpu.make_async_remote_copy(
        src_ref=tiles_ref,
        dst_ref=mbuf,
        send_sem=mirror_send,
        recv_sem=mirror_recv,
        device_id=mirror,
        device_id_type=MESH,
    )
    across.start()

    def send(s, carry):
        copy(s, 0).start()
        return carry

    lax.fori_loop(1, n, send, 0)
    rbuf[0] = tiles_ref[asked(0, base)]
    across.wait()

    def relay(s, carry):
        sbuf[n + s] = mbuf[asked(s, mirror_base)]
        return carry

    lax.fori_loop(1, n, relay, 0)

    def forward(s, carry):
        copy(s, 1).start()
        return carry

    lax.fori_loop(1, n, forward, 0)
    rbuf[n] = mbuf[asked(0, mirror_base)]

    def land(s, carry):
        copy(s, 0).wait()
        copy(s, 1).wait()
        return carry

    lax.fori_loop(1, n, land, 0)

    def find(owner):
        owner_row = lax.rem(owner, members)
        spot_of = owner // members * part + lax.rem(owner_row, part)
        return lax.rem(me - spot_of + n, n) + jnp.where(owner_row // part == half, 0, n)

    multiply(base, find, cols_ref, outs_ref, tiles_ref, rbuf, out_ref)


def same(lane, rows, groups, members):
    device = lane // rows
    inner = lax.rem(device, members)
    spot = lax.rem(inner, PLANE)
    return device // members, inner // PLANE, spot // 2, lax.rem(spot, 2)


def ones(mask):
    return jnp.where(mask, 1.0, 0.0)


def across(a, b):
    dims = (((1,), (1,)), ((), ()))
    return lax.dot_general(
        a.astype(jnp.bfloat16), b.astype(jnp.bfloat16), dims, preferred_element_type=jnp.float32
    )


def iota(shape, axis):
    return lax.broadcasted_iota(jnp.int32, shape, axis)


def steps(value, bounds):
    return sum((value >= b).astype(jnp.int32) for b in bounds)


def named_rows(cols, here, rows, groups, members):
    g, z, y, x = here
    lines = members // PLANE
    crowd = groups * PLANE
    total = cols.shape[1]
    devices = groups * members
    count = devices + 8
    query = iota((count, total), 0)
    lane = iota((count, total), 1)
    og, oz, oy, ox = same(lane, rows, groups, members)
    rel = PLANE * lax.rem(og + g, 2) + 2 * lax.rem(oy + y, 2) + lax.rem(ox + x, 2)
    up = lax.rem(oz - z + lines, lines)
    alone = (query < devices) & (up == query // crowd) & (rel == lax.rem(query, crowd))
    plane = up == query - devices
    group = ones(alone | plane)
    index = iota((total, total), 0)
    hits = jnp.zeros((count, total), jnp.float32)
    for k in range(cols.shape[0]):
        hits = hits + across(group, ones(index == cols[k : k + 1]))
    return ones(hits > 0.5)


def ranked(masks, upper):
    ranks = []
    before = jnp.zeros((masks[0].shape[0], 1), jnp.float32)
    for m in masks:
        ranks.append(across(m, upper) + before)
        before = before + jnp.sum(m, axis=1, keepdims=True)
    return masks, ranks, before


def slots(held, first, stride, bounds):
    masks, ranks, sums = held
    start = jnp.zeros((8, 1), jnp.float32)
    used, at = [0.0 for _ in masks], [0.0 for _ in masks]
    for k, bound in enumerate(bounds):
        b = 8 * (first + k * stride)
        start = jnp.maximum(start, float(bound))
        for j in range(len(masks)):
            m = masks[j][b : b + 8]
            used[j] = used[j] + m
            at[j] = at[j] + m * (start + ranks[j][b : b + 8])
        start = start + sums[b : b + 8]
    return used, at, start


def triangle(total):
    return ones(iota((total, total), 0) > iota((total, total), 1))


def column(slot, spot, count):
    hot = [ones(slot == spot[q : q + 1]) for q in range(count)]
    return jnp.concatenate(hot, axis=0)


def owned(cols, named, here, rows, groups, members):
    devices = groups * members
    total = cols.shape[1]
    per = cols.shape[0]
    wanted = ones(jnp.sum(named[devices : devices + 8], axis=0, keepdims=True) > 0.5)
    masks = [jnp.broadcast_to(wanted * ones(cols[j : j + 1] >= 0), (8, total)) for j in range(per)]
    a, b = iota((total, total), 0), iota((total, total), 1)
    block = a // rows == b // rows
    upper, whole = ones(block & (a > b)), ones(block)
    ranks = []
    before = jnp.zeros((8, total), jnp.float32)
    for m in masks:
        ranks.append(across(m, upper) + before)
        before = before + across(m, whole)
    lane = iota((8, total), 1)
    og, oz, oy, ox = same(lane, rows, groups, members)
    g, z, y, x = here
    mine = (og == g) & (oz == z) & (oy == y) & (ox == x)
    item = lax.rem(lane, rows)
    picks = jnp.zeros((8, 128), jnp.float32)
    slot = iota((128, total), 0)
    for j in range(per):
        spot = jnp.where(mine & (masks[j] > 0.5), ranks[j], -1.0).astype(jnp.int32)
        picks = picks + across((item * per + j).astype(jnp.float32), column(slot, spot, 1))
    picks = jnp.clip(picks.astype(jnp.int32), 0, rows * per - 1)
    return ranks, before, picks


def tables(cols, named, ranks_a, here, rows, groups, members):
    g, z, y, x = here
    lines = members // PLANE
    crowd = groups * PLANE
    devices = groups * members
    total = cols.shape[1]
    per = cols.shape[0]
    lane = iota((8, total), 1)
    sub = iota((8, total), 0)
    og, oz, oy, ox = same(lane, rows, groups, members)
    rel = PLANE * lax.rem(og + g, 2) + 2 * lax.rem(oy + y, 2) + lax.rem(ox + x, 2)
    local = oz == z
    back = lax.rem(z - oz + lines, lines)
    planes = named[devices : devices + 8]
    mine = jnp.broadcast_to(planes[0:1], (8, total))
    near = named[:crowd]
    upper = triangle(total)
    classes = range(len(START_B))
    present = [ones(cols[j : j + 1] >= 0) for j in range(per)]
    sends, takes = planes * ones(local), mine * ones(back == sub)
    stacks = []
    for j in range(per):
        lev = steps(ranks_a[j], CUT_A[1:-1])
        kept = [present[j] * ones(lev == k) for k in classes]
        stacks.append(jnp.concatenate([sends * m for m in kept] + [takes * m for m in kept], axis=0))
    held = ranked(stacks, upper)
    send_used, send_at, _ = slots(held, 0, 1, START_B)
    take_used, take_at, _ = slots(held, len(classes), 1, START_B)
    cap_a, cap_b, cap_c = CUT_A[-1], CUT_B[-1], CUT_C[-1]
    arena = crowd * cap_a
    first = (rel * cap_a).astype(jnp.float32)
    home = [first + jnp.minimum(ranks_a[j], cap_a - 1.0) for j in range(per)]
    offset = (arena + (sub - 1) * cap_b).astype(jnp.float32)
    arrived, mids = [], []
    for j in range(per):
        spot = jnp.sum(take_used[j] * take_at[j], axis=0, keepdims=True)
        far = jnp.sum(take_used[j] * (offset + take_at[j]), axis=0, keepdims=True)
        arrived.append(jnp.where(local, home[j], jnp.broadcast_to(far, (8, total))))
        part = jnp.where(local, 0, 1 + steps(jnp.broadcast_to(spot, (8, total)), PART_B))
        kept = near * present[j]
        mids.append(jnp.concatenate([kept * ones(part == c) for c in range(len(CUT_C) - 1)], axis=0))
    mid_used, mid_at, _ = slots(ranked(mids, upper), 0, 1, CUT_C[:-1])

    def sources(used, at, address, count):
        out = jnp.zeros((8, SPAN * count), jnp.float32)
        slot = iota((SPAN, total), 0)
        for j in range(per):
            spot = jnp.where(used[j] > 0.5, at[j], -1.0).astype(jnp.int32)
            out = out + across(address[j], column(slot, spot, count))
        return jnp.clip(out.astype(jnp.int32), 0, arena + (lines - 1) * cap_b - 1)

    b_list = sources(send_used, send_at, home, lines)
    c_list = sources(mid_used, mid_at, arrived, crowd)
    final = [jnp.clip(mid_at[j][0:1].astype(jnp.int32), 0, cap_c - 1) for j in range(per)]
    lines_out = []
    for block in [b_list[0:1], c_list[0:1]] + final:
        width = block.shape[1]
        if width % 128:
            block = jnp.concatenate([block, jnp.zeros((1, -width % 128), jnp.int32)], axis=1)
        for h in range(-(-width // 128)):
            lines_out.append(block[:, 128 * h : 128 * h + 128])
    lines_out.append(jnp.zeros((TABLE - len(lines_out), 128), jnp.int32))
    return jnp.concatenate(lines_out, axis=0)


def overflow(cols, named, ranks_a, loads_a, here, rows, groups, members):
    g, z, y, x = here
    lines = members // PLANE
    crowd = groups * PLANE
    devices = groups * members
    total = cols.shape[1]
    per = cols.shape[0]
    lane = iota((8, total), 1)
    oz = lax.rem(lane // rows, members) // PLANE
    up = lax.rem(oz - z + lines, lines)
    planes = named[devices : devices + 8]
    classes = range(len(START_B))
    present = [ones(cols[j : j + 1] >= 0) for j in range(per)]
    stacks = []
    for j in range(per):
        lev = steps(ranks_a[j], CUT_A[1:-1])
        kept = planes * present[j]
        stacks.append(
            jnp.concatenate(
                [kept * ones((up == s) & (lev == k)) for k in classes for s in range(lines)], axis=0
            )
        )
    held = ranked(stacks, triangle(total))
    sub = iota((8, 1), 0)
    worst = jnp.maximum(jnp.max(loads_a, axis=1, keepdims=True) - CUT_A[-1], 0.0)
    at = [0.0 for _ in range(per)]
    for s in range(lines):
        _, spot, end = slots(held, s, lines, START_B)
        worst = jnp.maximum(worst, jnp.where((sub < lines) & (sub != s), end - CUT_B[-1], 0.0))
        for j in range(per):
            at[j] = at[j] + spot[j]
    for q in range(lines):
        near = named[crowd * q : crowd * (q + 1)]
        sums = [jnp.zeros((8, 1), jnp.float32) for _ in CUT_C[:-1]]
        for j in range(per):
            load = near * present[j]
            spot = jnp.broadcast_to(at[j][q : q + 1], (8, total))
            part = jnp.where(up == q, 0, 1 + steps(spot, PART_B))
            for c in range(len(sums)):
                sums[c] = sums[c] + jnp.sum(load * ones(part == c), axis=1, keepdims=True)
        end = jnp.zeros((8, 1), jnp.float32)
        for bound, n in zip(CUT_C, sums):
            end = jnp.maximum(end, float(bound)) + n
        worst = jnp.maximum(worst, end - CUT_C[-1])
    return jnp.max(worst).astype(jnp.int32)


def compact_kernel(
    groups, members, cols_hbm, outs_hbm, tiles_hbm, out_ref, over_ref, cols_vec, outs_vec,
    cols_ref, outs_ref, tiles, a_send, parts, arena, b_send, b_recv, c_send, c_recv,
    own_vec, own, tab_vec, tab, load_sem, tab_sem, a_out, a_in, b_out, b_in, c_out, c_in,
):
    rows, per, side, _ = tiles.shape
    lines = members // PLANE
    crowd = groups * PLANE
    piece = side // crowd
    g, row = lax.axis_index("grp"), lax.axis_index("row")
    z, spot = row // PLANE, lax.rem(row, PLANE)
    y, x = spot // 2, lax.rem(spot, 2)
    here = (g, z, y, x)
    base = (g * members + row) * rows
    me = g * PLANE + spot
    stages, cap_a, cap_b = len(CUT_A) - 1, CUT_A[-1], CUT_B[-1]
    chunks_b, chunks_c = len(CUT_B) - 1, len(CUT_C) - 1

    def near_device(u):
        dg, dy, dx = u // PLANE, u // 2 % 2, u % 2
        ns = 2 * lax.rem(y + dy, 2) + lax.rem(x + dx, 2)
        return {"grp": lax.rem(g + dg, 2), "row": z * PLANE + ns}

    def line_device(dz):
        return {"grp": g, "row": lax.rem(z + dz, lines) * PLANE + spot}

    barrier = pltpu.get_barrier_semaphore()
    for dz in range(1, lines):
        pl.semaphore_signal(barrier, inc=1, device_id=line_device(dz), device_id_type=MESH)
    for u in range(crowd - 1, 0, -1):
        pl.semaphore_signal(barrier, inc=1, device_id=near_device(u), device_id_type=MESH)
    loads = [
        pltpu.make_async_copy(cols_hbm, cols_vec, load_sem.at[0]),
        pltpu.make_async_copy(tiles_hbm, tiles, load_sem.at[1]),
        pltpu.make_async_copy(cols_hbm, cols_ref, load_sem.at[2]),
        pltpu.make_async_copy(outs_hbm, outs_ref, load_sem.at[3]),
        pltpu.make_async_copy(outs_hbm, outs_vec, load_sem.at[4]),
    ]
    for load in loads:
        load.start()
    loads[0].wait()
    cols = cols_vec[...]
    named = named_rows(cols, here, rows, groups, members)
    ranks_a, loads_a, picks = owned(cols, named, here, rows, groups, members)
    own_vec[...] = picks
    move = pltpu.make_async_copy(own_vec, own, tab_sem.at[0])
    move.start()
    for load in loads[1:]:
        load.wait()
    move.wait()
    for q in range(cap_a):
        pick = own[0, q]
        a_send[q] = tiles[pick // per, lax.rem(pick, per)]
    pl.semaphore_wait(barrier, lines - 1 + crowd - 1)

    def a_copy(u, k):
        there = near_device(u)
        start = pl.multiple_of((there["grp"] * PLANE + lax.rem(there["row"], PLANE)) * piece, piece)
        span = pl.ds(CUT_A[k], CUT_A[k + 1] - CUT_A[k])
        return pltpu.make_async_remote_copy(
            src_ref=a_send.at[span, pl.ds(start, piece), :],
            dst_ref=parts.at[u, span],
            send_sem=a_out.at[stages * u + k],
            recv_sem=a_in.at[stages * u + k],
            device_id=there,
            device_id_type=MESH,
        )

    order = [7, 3, 5, 6, 1, 2, 4]
    for k in range(stages):
        for u in order:
            a_copy(u, k).start()

    tab_vec[...] = tables(cols, named, ranks_a, here, rows, groups, members)
    move = pltpu.make_async_copy(tab_vec, tab, tab_sem.at[1])
    move.start()
    mine = pl.multiple_of(me * piece, piece)
    for q in range(cap_a):
        arena[q] = a_send[q, pl.ds(mine, piece), :]
    move.wait()

    def pick(options):
        value = jnp.int32(options[0])
        for at, option in enumerate(options[1:]):
            value = jnp.where(z == at + 1, option, value)
        return value

    far_first = [pick((3, 2, 2, 1)), pick((2, 1, 3, 2)), pick((1, 3, 1, 3))]

    def b_copy(k, dz):
        span = pl.ds(CUT_B[k], CUT_B[k + 1] - CUT_B[k])
        return pltpu.make_async_remote_copy(
            src_ref=b_send.at[dz - 1, span],
            dst_ref=b_recv.at[dz - 1, span],
            send_sem=b_out.at[chunks_b * (dz - 1) + k],
            recv_sem=b_in.at[chunks_b * (dz - 1) + k],
            device_id=line_device(dz),
            device_id_type=MESH,
        )

    def c_copy(k, u):
        span = pl.ds(CUT_C[k], CUT_C[k + 1] - CUT_C[k])
        return pltpu.make_async_remote_copy(
            src_ref=c_send.at[u, span],
            dst_ref=c_recv.at[u, span],
            send_sem=c_out.at[chunks_c * u + k],
            recv_sem=c_in.at[chunks_c * u + k],
            device_id=near_device(u),
            device_id_type=MESH,
        )

    wide_b, wide_c = -(-lines * SPAN // 128), -(-crowd * SPAN // 128)

    def entry(first, at):
        return tab[first + at // 128, at % 128]

    def push_b(k):
        for dz in range(1, lines):
            for q in range(CUT_B[k], CUT_B[k + 1]):
                b_send[dz - 1, q] = arena[entry(0, SPAN * dz + q)]
        for dz in far_first:
            b_copy(k, dz).start()

    def push_c(k):
        for u in order + [0]:
            for q in range(CUT_C[k], CUT_C[k + 1]):
                tile = arena[entry(wide_b, SPAN * u + q)]
                if u:
                    c_send[u, q] = tile
                else:
                    c_recv[0, q] = tile
        for core in range(groups):
            side_of = PLANE * lax.rem(core - g + groups, groups)
            for at in (3, 1, 2):
                c_copy(k, side_of + at).start()
        c_copy(k, PLANE).start()

    for k in range(stages):
        for u in order:
            a_copy(u, k).wait_recv()
            for q in range(CUT_A[k], CUT_A[k + 1]):
                arena[u * cap_a + q] = parts[u, q]
        for part in range(chunks_b):
            if CLASS_B[part] == k:
                push_b(part)
    push_c(0)
    over_ref[0] = overflow(cols, named, ranks_a, loads_a, here, rows, groups, members)
    held = crowd * cap_a
    sent = 1
    for k in range(chunks_b):
        for dz in range(1, lines):
            b_copy(k, dz).wait_recv()
            for q in range(CUT_B[k], CUT_B[k + 1]):
                arena[held + (dz - 1) * cap_b + q] = b_recv[dz - 1, q]
        if CUT_B[k + 1] in PART_B or k == chunks_b - 1:
            push_c(sent)
            sent += 1

    sources = []
    for piece_of in range(crowd):
        pg, ps = piece_of // PLANE, piece_of % PLANE
        dy, dx = lax.rem(ps // 2 + y, 2), lax.rem(ps % 2 + x, 2)
        sources.append(PLANE * lax.rem(pg + g, 2) + 2 * dy + dx)
    for u in order:
        for k in range(stages):
            a_copy(u, k).wait_send()
        for k in range(chunks_c):
            c_copy(k, u).wait_send()
    for dz in range(1, lines):
        for k in range(chunks_b):
            b_copy(k, dz).wait_send()
    outs_row = outs_ref.shape[0]
    wide = cols_ref.shape[1] // 128
    picks = {}
    for i in range(rows):
        for k in range(per):
            c = cols_ref[k, base + i]
            safe = jnp.maximum(c, 0)
            for p in range(outs_row):
                o = outs_ref[p, i]
                which = jnp.int32(0)
                hit = jnp.int32(0)
                for j in range(per):
                    match = cols_ref[j, safe] == o
                    which = jnp.where(match, j, which)
                    hit = jnp.where(match & (c >= 0), 1, hit)
                slot = tab[wide_b + wide_c + wide * which + safe // 128, lax.rem(safe, 128)]
                picks[i, k, p] = slot, hit
    for k in range(chunks_c):
        for u in order:
            c_copy(k, u).wait_recv()

    for i in range(rows):
        left = jnp.concatenate([tiles[i, k] for k in range(per)], axis=1)
        stack = []
        for k in range(per):
            line = []
            for p in range(outs_row):
                slot, hit = picks[i, k, p]
                tile = jnp.concatenate([c_recv[s, slot] for s in sources], axis=0)
                line.append(tile * hit.astype(jnp.float32).astype(jnp.bfloat16))
            stack.append(jnp.concatenate(line, axis=1))
        right = jnp.concatenate(stack, axis=0)
        prod = jnp.dot(left, right, preferred_element_type=jnp.float32).astype(jnp.bfloat16)
        for p in range(outs_row):
            out_ref[i, p] = prod[:, p * side : (p + 1) * side]


def params(identity):
    return pltpu.CompilerParams(
        collective_id=identity, has_side_effects=True, vmem_limit_bytes=56 * 1024 * 1024
    )


def shards(block_tiles, tile_columns, requests, output_columns):
    groups = lax.axis_size("grp")
    members = lax.axis_size("row")
    n = groups * members
    rows, per_row, side, _ = block_tiles.shape
    vmem = pl.BlockSpec(memory_space=pltpu.VMEM)
    smem = pl.BlockSpec(memory_space=pltpu.SMEM)
    out = jax.ShapeDtypeStruct((rows, output_columns.shape[1], side, side), jnp.bfloat16)
    tile_rows = lambda count: pltpu.VMEM((count, per_row, side, side), jnp.bfloat16)
    columns, outs = tile_columns.T, output_columns.T

    def dense():
        return pl.pallas_call(
            functools.partial(dense_kernel, groups, members),
            out_shape=out,
            in_specs=[smem, smem, vmem],
            out_specs=vmem,
            scratch_shapes=[
                tile_rows(n),
                tile_rows(n),
                tile_rows(rows),
                pltpu.SemaphoreType.DMA((n,)),
                pltpu.SemaphoreType.DMA((n,)),
                pltpu.SemaphoreType.DMA,
                pltpu.SemaphoreType.DMA,
            ],
            compiler_params=params(0),
        )(columns, outs, block_tiles)

    lines = members // PLANE
    crowd = groups * PLANE
    cap_b, cap_c = CUT_B[-1], CUT_C[-1]
    held = crowd * CUT_A[-1] + (lines - 1) * cap_b
    fits = groups == 2 and members == 4 * PLANE and per_row == 2 and CUT_A[-1] <= 128
    fits = fits and tile_columns.shape[0] % 128 == 0 and side % (16 * crowd) == 0 and held <= 256
    if not fits:
        return dense()
    piece = side // crowd
    pieces = lambda *lead: pltpu.VMEM((*lead, piece, side), jnp.bfloat16)
    dma = pltpu.SemaphoreType.DMA
    hbm = pl.BlockSpec(memory_space=pl.ANY)
    stages, chunks_b, chunks_c = len(CUT_A) - 1, len(CUT_B) - 1, len(CUT_C) - 1
    like = lambda array: jax.ShapeDtypeStruct(array.shape, array.dtype)
    compact, over, columns, outs = pl.pallas_call(
        functools.partial(compact_kernel, groups, members),
        out_shape=(out, jax.ShapeDtypeStruct((1,), jnp.int32), like(columns), like(outs)),
        in_specs=[hbm, hbm, hbm],
        out_specs=(vmem, smem, vmem, vmem),
        scratch_shapes=[
            pltpu.SMEM(columns.shape, jnp.int32),
            pltpu.SMEM(outs.shape, jnp.int32),
            pltpu.VMEM(block_tiles.shape, jnp.bfloat16),
            pltpu.VMEM((CUT_A[-1], side, side), jnp.bfloat16),
            pieces(crowd, CUT_A[-1]),
            pieces(held),
            pieces(lines - 1, cap_b),
            pieces(lines - 1, cap_b),
            pieces(crowd, cap_c),
            pieces(crowd, cap_c),
            pltpu.VMEM((8, 128), jnp.int32),
            pltpu.SMEM((8, 128), jnp.int32),
            pltpu.VMEM((TABLE, 128), jnp.int32),
            pltpu.SMEM((TABLE, 128), jnp.int32),
            dma((5,)),
            dma((2,)),
            dma((stages * crowd,)),
            dma((stages * crowd,)),
            dma((chunks_b * (lines - 1),)),
            dma((chunks_b * (lines - 1),)),
            dma((chunks_c * crowd,)),
            dma((chunks_c * crowd,)),
        ],
        compiler_params=params(1),
    )(columns, outs, block_tiles)
    return lax.cond(over[0] > 0, dense, lambda: compact)


def solution(mesh):
    placed = (
        P(("grp", "row"), None, None, None),
        P(),
        P(("grp", "row"), None),
        P(("grp", "row"), None),
    )
    return jax.shard_map(
        shards,
        mesh=mesh,
        in_specs=placed,
        out_specs=P(("grp", "row"), None, None, None),
        check_vma=False,
    )
```

```python
import functools

import jax
import jax.numpy as jnp
from jax import lax
from jax.experimental import pallas as pl
from jax.experimental.pallas import tpu as pltpu
from jax.sharding import PartitionSpec as P

MESH = pl.DeviceIdType.MESH
PLANE = 4
CUT_A = (0, 2, 6, 12)
START_B = (0, 6, 20)
CUT_B = (0, 6, 20, 32)
CLASS_B = (0, 1, 2)
PART_B = (6, 20)
CUT_C = (0, 3, 7, 16, 21)
SPAN = 40
TABLE = 16


def multiply(base, find, cols_ref, outs_ref, tiles_ref, rbuf, out_ref):
    rows, per_row, side, _ = tiles_ref.shape
    outs_row = outs_ref.shape[0]
    for i in range(rows):
        left = jnp.concatenate([tiles_ref[i, k] for k in range(per_row)], axis=1)
        stack = []
        for k in range(per_row):
            c = cols_ref[k, base + i]
            safe = jnp.maximum(c, 0)
            slot = find(safe // rows)
            line = []
            for p in range(outs_row):
                o = outs_ref[p, i]
                which = jnp.int32(0)
                hit = jnp.int32(0)
                for j in range(per_row):
                    same = cols_ref[j, safe] == o
                    which = jnp.where(same, j, which)
                    hit = jnp.where(same & (c >= 0), 1, hit)
                tile = rbuf[slot, which]
                line.append(tile * hit.astype(jnp.float32).astype(jnp.bfloat16))
            stack.append(jnp.concatenate(line, axis=1))
        right = jnp.concatenate(stack, axis=0)
        prod = jnp.dot(left, right, preferred_element_type=jnp.float32).astype(jnp.bfloat16)
        for p in range(outs_row):
            out_ref[i, p] = prod[:, p * side : (p + 1) * side]


def dense_kernel(
    groups, members, cols_ref, outs_ref, tiles_ref, out_ref,
    sbuf, rbuf, mbuf, send_sem, recv_sem, mirror_send, mirror_recv,
):
    part = members // 2
    n = groups * part
    rows, per_row, side, _ = tiles_ref.shape
    grp, row = lax.axis_index("grp"), lax.axis_index("row")
    half, spot = row // part, lax.rem(row, part)
    me = grp * part + spot
    base = (grp * members + row) * rows
    mirror_row = (1 - half) * part + spot
    mirror = {"grp": grp, "row": mirror_row}
    mirror_base = (grp * members + mirror_row) * rows

    def place(s):
        u = lax.rem(me + s, n)
        return u // part, half * part + lax.rem(u, part)

    def target(s):
        g, r = place(s)
        return {"grp": g, "row": r}

    barrier = pltpu.get_barrier_semaphore()
    pl.semaphore_signal(barrier, inc=1, device_id=mirror, device_id_type=MESH)

    def greet(s, carry):
        pl.semaphore_signal(barrier, inc=1, device_id=target(s), device_id_type=MESH)
        return carry

    lax.fori_loop(1, n, greet, 0)

    def asked(s, start):
        g, r = place(s)
        first = (g * members + r) * rows
        t = jnp.int32(0)
        for i in range(rows):
            for k in range(per_row):
                c = cols_ref[k, first + i] - start
                t = jnp.where((c >= 0) & (c < rows), c, t)
        return t

    def copy(s, level):
        return pltpu.make_async_remote_copy(
            src_ref=sbuf.at[level * n + s],
            dst_ref=rbuf.at[level * n + s],
            send_sem=send_sem.at[level * n + s],
            recv_sem=recv_sem.at[level * n + s],
            device_id=target(s),
            device_id_type=MESH,
        )

    def pack(s, carry):
        sbuf[s] = tiles_ref[asked(s, base)]
        return carry

    lax.fori_loop(1, n, pack, 0)
    pl.semaphore_wait(barrier, n)
    across = pltpu.make_async_remote_copy(
        src_ref=tiles_ref,
        dst_ref=mbuf,
        send_sem=mirror_send,
        recv_sem=mirror_recv,
        device_id=mirror,
        device_id_type=MESH,
    )
    across.start()

    def send(s, carry):
        copy(s, 0).start()
        return carry

    lax.fori_loop(1, n, send, 0)
    rbuf[0] = tiles_ref[asked(0, base)]
    across.wait()

    def relay(s, carry):
        sbuf[n + s] = mbuf[asked(s, mirror_base)]
        return carry

    lax.fori_loop(1, n, relay, 0)

    def forward(s, carry):
        copy(s, 1).start()
        return carry

    lax.fori_loop(1, n, forward, 0)
    rbuf[n] = mbuf[asked(0, mirror_base)]

    def land(s, carry):
        copy(s, 0).wait()
        copy(s, 1).wait()
        return carry

    lax.fori_loop(1, n, land, 0)

    def find(owner):
        owner_row = lax.rem(owner, members)
        spot_of = owner // members * part + lax.rem(owner_row, part)
        return lax.rem(me - spot_of + n, n) + jnp.where(owner_row // part == half, 0, n)

    multiply(base, find, cols_ref, outs_ref, tiles_ref, rbuf, out_ref)


def same(lane, rows, groups, members):
    device = lane // rows
    inner = lax.rem(device, members)
    spot = lax.rem(inner, PLANE)
    return device // members, inner // PLANE, spot // 2, lax.rem(spot, 2)


def ones(mask):
    return jnp.where(mask, 1.0, 0.0)


def across(a, b):
    dims = (((1,), (1,)), ((), ()))
    return lax.dot_general(
        a.astype(jnp.bfloat16), b.astype(jnp.bfloat16), dims, preferred_element_type=jnp.float32
    )


def iota(shape, axis):
    return lax.broadcasted_iota(jnp.int32, shape, axis)


def steps(value, bounds):
    return sum((value >= b).astype(jnp.int32) for b in bounds)


def named_rows(cols, here, rows, groups, members):
    g, z, y, x = here
    lines = members // PLANE
    crowd = groups * PLANE
    total = cols.shape[1]
    devices = groups * members
    count = devices + 8
    query = iota((count, total), 0)
    lane = iota((count, total), 1)
    og, oz, oy, ox = same(lane, rows, groups, members)
    rel = PLANE * lax.rem(og + g, 2) + 2 * lax.rem(oy + y, 2) + lax.rem(ox + x, 2)
    up = lax.rem(oz - z + lines, lines)
    alone = (query < devices) & (up == query // crowd) & (rel == lax.rem(query, crowd))
    plane = up == query - devices
    group = ones(alone | plane)
    index = iota((total, total), 0)
    hits = jnp.zeros((count, total), jnp.float32)
    for k in range(cols.shape[0]):
        hits = hits + across(group, ones(index == cols[k : k + 1]))
    return ones(hits > 0.5)


def ranked(masks, upper):
    ranks = []
    before = jnp.zeros((masks[0].shape[0], 1), jnp.float32)
    for m in masks:
        ranks.append(across(m, upper) + before)
        before = before + jnp.sum(m, axis=1, keepdims=True)
    return masks, ranks, before


def slots(held, first, stride, bounds):
    masks, ranks, sums = held
    start = jnp.zeros((8, 1), jnp.float32)
    used, at = [0.0 for _ in masks], [0.0 for _ in masks]
    for k, bound in enumerate(bounds):
        b = 8 * (first + k * stride)
        start = jnp.maximum(start, float(bound))
        for j in range(len(masks)):
            m = masks[j][b : b + 8]
            used[j] = used[j] + m
            at[j] = at[j] + m * (start + ranks[j][b : b + 8])
        start = start + sums[b : b + 8]
    return used, at, start


def triangle(total):
    return ones(iota((total, total), 0) > iota((total, total), 1))


def column(slot, spot, count):
    hot = [ones(slot == spot[q : q + 1]) for q in range(count)]
    return jnp.concatenate(hot, axis=0)


def owned(cols, named, here, rows, groups, members):
    devices = groups * members
    total = cols.shape[1]
    per = cols.shape[0]
    wanted = ones(jnp.sum(named[devices : devices + 8], axis=0, keepdims=True) > 0.5)
    masks = [jnp.broadcast_to(wanted * ones(cols[j : j + 1] >= 0), (8, total)) for j in range(per)]
    a, b = iota((total, total), 0), iota((total, total), 1)
    block = a // rows == b // rows
    upper, whole = ones(block & (a > b)), ones(block)
    ranks = []
    before = jnp.zeros((8, total), jnp.float32)
    for m in masks:
        ranks.append(across(m, upper) + before)
        before = before + across(m, whole)
    lane = iota((8, total), 1)
    og, oz, oy, ox = same(lane, rows, groups, members)
    g, z, y, x = here
    mine = (og == g) & (oz == z) & (oy == y) & (ox == x)
    item = lax.rem(lane, rows)
    picks = jnp.zeros((8, 128), jnp.float32)
    slot = iota((128, total), 0)
    for j in range(per):
        spot = jnp.where(mine & (masks[j] > 0.5), ranks[j], -1.0).astype(jnp.int32)
        picks = picks + across((item * per + j).astype(jnp.float32), column(slot, spot, 1))
    picks = jnp.clip(picks.astype(jnp.int32), 0, rows * per - 1)
    return ranks, before, picks


def tables(cols, named, ranks_a, here, rows, groups, members):
    g, z, y, x = here
    lines = members // PLANE
    crowd = groups * PLANE
    devices = groups * members
    total = cols.shape[1]
    per = cols.shape[0]
    lane = iota((8, total), 1)
    sub = iota((8, total), 0)
    og, oz, oy, ox = same(lane, rows, groups, members)
    rel = PLANE * lax.rem(og + g, 2) + 2 * lax.rem(oy + y, 2) + lax.rem(ox + x, 2)
    local = oz == z
    back = lax.rem(z - oz + lines, lines)
    planes = named[devices : devices + 8]
    mine = jnp.broadcast_to(planes[0:1], (8, total))
    near = named[:crowd]
    upper = triangle(total)
    classes = range(len(START_B))
    present = [ones(cols[j : j + 1] >= 0) for j in range(per)]
    sends, takes = planes * ones(local), mine * ones(back == sub)
    stacks = []
    for j in range(per):
        lev = steps(ranks_a[j], CUT_A[1:-1])
        kept = [present[j] * ones(lev == k) for k in classes]
        stacks.append(jnp.concatenate([sends * m for m in kept] + [takes * m for m in kept], axis=0))
    held = ranked(stacks, upper)
    send_used, send_at, _ = slots(held, 0, 1, START_B)
    take_used, take_at, _ = slots(held, len(classes), 1, START_B)
    cap_a, cap_b, cap_c = CUT_A[-1], CUT_B[-1], CUT_C[-1]
    arena = crowd * cap_a
    first = (rel * cap_a).astype(jnp.float32)
    home = [first + jnp.minimum(ranks_a[j], cap_a - 1.0) for j in range(per)]
    offset = (arena + (sub - 1) * cap_b).astype(jnp.float32)
    arrived, mids = [], []
    for j in range(per):
        spot = jnp.sum(take_used[j] * take_at[j], axis=0, keepdims=True)
        far = jnp.sum(take_used[j] * (offset + take_at[j]), axis=0, keepdims=True)
        arrived.append(jnp.where(local, home[j], jnp.broadcast_to(far, (8, total))))
        part = jnp.where(local, 0, 1 + steps(jnp.broadcast_to(spot, (8, total)), PART_B))
        kept = near * present[j]
        mids.append(jnp.concatenate([kept * ones(part == c) for c in range(len(CUT_C) - 1)], axis=0))
    mid_used, mid_at, _ = slots(ranked(mids, upper), 0, 1, CUT_C[:-1])

    def sources(used, at, address, count):
        out = jnp.zeros((8, SPAN * count), jnp.float32)
        slot = iota((SPAN, total), 0)
        for j in range(per):
            spot = jnp.where(used[j] > 0.5, at[j], -1.0).astype(jnp.int32)
            out = out + across(address[j], column(slot, spot, count))
        return jnp.clip(out.astype(jnp.int32), 0, arena + (lines - 1) * cap_b - 1)

    b_list = sources(send_used, send_at, home, lines)
    c_list = sources(mid_used, mid_at, arrived, crowd)
    final = [jnp.clip(mid_at[j][0:1].astype(jnp.int32), 0, cap_c - 1) for j in range(per)]
    lines_out = []
    for block in [b_list[0:1], c_list[0:1]] + final:
        width = block.shape[1]
        if width % 128:
            block = jnp.concatenate([block, jnp.zeros((1, -width % 128), jnp.int32)], axis=1)
        for h in range(-(-width // 128)):
            lines_out.append(block[:, 128 * h : 128 * h + 128])
    lines_out.append(jnp.zeros((TABLE - len(lines_out), 128), jnp.int32))
    return jnp.concatenate(lines_out, axis=0)


def overflow(cols, named, ranks_a, loads_a, here, rows, groups, members):
    g, z, y, x = here
    lines = members // PLANE
    crowd = groups * PLANE
    devices = groups * members
    total = cols.shape[1]
    per = cols.shape[0]
    lane = iota((8, total), 1)
    oz = lax.rem(lane // rows, members) // PLANE
    up = lax.rem(oz - z + lines, lines)
    planes = named[devices : devices + 8]
    classes = range(len(START_B))
    present = [ones(cols[j : j + 1] >= 0) for j in range(per)]
    stacks = []
    for j in range(per):
        lev = steps(ranks_a[j], CUT_A[1:-1])
        kept = planes * present[j]
        stacks.append(
            jnp.concatenate(
                [kept * ones((up == s) & (lev == k)) for k in classes for s in range(lines)], axis=0
            )
        )
    held = ranked(stacks, triangle(total))
    sub = iota((8, 1), 0)
    worst = jnp.maximum(jnp.max(loads_a, axis=1, keepdims=True) - CUT_A[-1], 0.0)
    at = [0.0 for _ in range(per)]
    for s in range(lines):
        _, spot, end = slots(held, s, lines, START_B)
        worst = jnp.maximum(worst, jnp.where((sub < lines) & (sub != s), end - CUT_B[-1], 0.0))
        for j in range(per):
            at[j] = at[j] + spot[j]
    for q in range(lines):
        near = named[crowd * q : crowd * (q + 1)]
        sums = [jnp.zeros((8, 1), jnp.float32) for _ in CUT_C[:-1]]
        for j in range(per):
            load = near * present[j]
            spot = jnp.broadcast_to(at[j][q : q + 1], (8, total))
            part = jnp.where(up == q, 0, 1 + steps(spot, PART_B))
            for c in range(len(sums)):
                sums[c] = sums[c] + jnp.sum(load * ones(part == c), axis=1, keepdims=True)
        end = jnp.zeros((8, 1), jnp.float32)
        for bound, n in zip(CUT_C, sums):
            end = jnp.maximum(end, float(bound)) + n
        worst = jnp.maximum(worst, end - CUT_C[-1])
    return jnp.max(worst).astype(jnp.int32)


def compact_kernel(
    groups, members, cols_hbm, outs_hbm, tiles_hbm, out_ref, over_ref, cols_vec, outs_vec,
    cols_ref, outs_ref, tiles, a_send, parts, arena, b_send, b_recv, c_send, c_recv,
    own_vec, own, tab_vec, tab, load_sem, tab_sem, a_out, a_in, b_out, b_in, c_out, c_in,
):
    rows, per, side, _ = tiles.shape
    lines = members // PLANE
    crowd = groups * PLANE
    piece = side // crowd
    g, row = lax.axis_index("grp"), lax.axis_index("row")
    z, spot = row // PLANE, lax.rem(row, PLANE)
    y, x = spot // 2, lax.rem(spot, 2)
    here = (g, z, y, x)
    base = (g * members + row) * rows
    me = g * PLANE + spot
    stages, cap_a, cap_b = len(CUT_A) - 1, CUT_A[-1], CUT_B[-1]
    chunks_b, chunks_c = len(CUT_B) - 1, len(CUT_C) - 1

    def near_device(u):
        dg, dy, dx = u // PLANE, u // 2 % 2, u % 2
        ns = 2 * lax.rem(y + dy, 2) + lax.rem(x + dx, 2)
        return {"grp": lax.rem(g + dg, 2), "row": z * PLANE + ns}

    def line_device(dz):
        return {"grp": g, "row": lax.rem(z + dz, lines) * PLANE + spot}

    barrier = pltpu.get_barrier_semaphore()
    for dz in range(1, lines):
        pl.semaphore_signal(barrier, inc=1, device_id=line_device(dz), device_id_type=MESH)
    for u in range(crowd - 1, 0, -1):
        pl.semaphore_signal(barrier, inc=1, device_id=near_device(u), device_id_type=MESH)
    loads = [
        pltpu.make_async_copy(cols_hbm, cols_vec, load_sem.at[0]),
        pltpu.make_async_copy(tiles_hbm, tiles, load_sem.at[1]),
        pltpu.make_async_copy(cols_hbm, cols_ref, load_sem.at[2]),
        pltpu.make_async_copy(outs_hbm, outs_ref, load_sem.at[3]),
        pltpu.make_async_copy(outs_hbm, outs_vec, load_sem.at[4]),
    ]
    for load in loads:
        load.start()
    loads[0].wait()
    cols = cols_vec[...]
    named = named_rows(cols, here, rows, groups, members)
    ranks_a, loads_a, picks = owned(cols, named, here, rows, groups, members)
    own_vec[...] = picks
    move = pltpu.make_async_copy(own_vec, own, tab_sem.at[0])
    move.start()
    for load in loads[1:]:
        load.wait()
    move.wait()
    for q in range(cap_a):
        pick = own[0, q]
        a_send[q] = tiles[pick // per, lax.rem(pick, per)]
    pl.semaphore_wait(barrier, lines - 1 + crowd - 1)

    def a_copy(u, k):
        there = near_device(u)
        start = pl.multiple_of((there["grp"] * PLANE + lax.rem(there["row"], PLANE)) * piece, piece)
        span = pl.ds(CUT_A[k], CUT_A[k + 1] - CUT_A[k])
        return pltpu.make_async_remote_copy(
            src_ref=a_send.at[span, pl.ds(start, piece), :],
            dst_ref=parts.at[u, span],
            send_sem=a_out.at[stages * u + k],
            recv_sem=a_in.at[stages * u + k],
            device_id=there,
            device_id_type=MESH,
        )

    order = [7, 3, 5, 6, 1, 2, 4]
    for k in range(stages):
        for u in order:
            a_copy(u, k).start()

    tab_vec[...] = tables(cols, named, ranks_a, here, rows, groups, members)
    move = pltpu.make_async_copy(tab_vec, tab, tab_sem.at[1])
    move.start()
    mine = pl.multiple_of(me * piece, piece)
    for q in range(cap_a):
        arena[q] = a_send[q, pl.ds(mine, piece), :]
    move.wait()

    def pick(options):
        value = jnp.int32(options[0])
        for at, option in enumerate(options[1:]):
            value = jnp.where(z == at + 1, option, value)
        return value

    far_first = [pick((3, 2, 2, 1)), pick((2, 1, 3, 2)), pick((1, 3, 1, 3))]

    def b_copy(k, dz):
        span = pl.ds(CUT_B[k], CUT_B[k + 1] - CUT_B[k])
        return pltpu.make_async_remote_copy(
            src_ref=b_send.at[dz - 1, span],
            dst_ref=b_recv.at[dz - 1, span],
            send_sem=b_out.at[chunks_b * (dz - 1) + k],
            recv_sem=b_in.at[chunks_b * (dz - 1) + k],
            device_id=line_device(dz),
            device_id_type=MESH,
        )

    def c_copy(k, u):
        span = pl.ds(CUT_C[k], CUT_C[k + 1] - CUT_C[k])
        return pltpu.make_async_remote_copy(
            src_ref=c_send.at[u, span],
            dst_ref=c_recv.at[u, span],
            send_sem=c_out.at[chunks_c * u + k],
            recv_sem=c_in.at[chunks_c * u + k],
            device_id=near_device(u),
            device_id_type=MESH,
        )

    wide_b, wide_c = -(-lines * SPAN // 128), -(-crowd * SPAN // 128)

    def entry(first, at):
        return tab[first + at // 128, at % 128]

    def push_b(k):
        for dz in range(1, lines):
            for q in range(CUT_B[k], CUT_B[k + 1]):
                b_send[dz - 1, q] = arena[entry(0, SPAN * dz + q)]
        for dz in far_first:
            b_copy(k, dz).start()

    def push_c(k):
        for u in order + [0]:
            for q in range(CUT_C[k], CUT_C[k + 1]):
                tile = arena[entry(wide_b, SPAN * u + q)]
                if u:
                    c_send[u, q] = tile
                else:
                    c_recv[0, q] = tile
        for core in range(groups):
            side_of = PLANE * lax.rem(core - g + groups, groups)
            for at in (3, 1, 2):
                c_copy(k, side_of + at).start()
        c_copy(k, PLANE).start()

    for k in range(stages):
        for u in order:
            a_copy(u, k).wait_recv()
            for q in range(CUT_A[k], CUT_A[k + 1]):
                arena[u * cap_a + q] = parts[u, q]
        for part in range(chunks_b):
            if CLASS_B[part] == k:
                push_b(part)
    push_c(0)
    over_ref[0] = overflow(cols, named, ranks_a, loads_a, here, rows, groups, members)
    held = crowd * cap_a
    sent = 1
    for k in range(chunks_b):
        for dz in range(1, lines):
            b_copy(k, dz).wait_recv()
            for q in range(CUT_B[k], CUT_B[k + 1]):
                arena[held + (dz - 1) * cap_b + q] = b_recv[dz - 1, q]
        if CUT_B[k + 1] in PART_B or k == chunks_b - 1:
            push_c(sent)
            sent += 1

    sources = []
    for piece_of in range(crowd):
        pg, ps = piece_of // PLANE, piece_of % PLANE
        dy, dx = lax.rem(ps // 2 + y, 2), lax.rem(ps % 2 + x, 2)
        sources.append(PLANE * lax.rem(pg + g, 2) + 2 * dy + dx)
    for u in order:
        for k in range(stages):
            a_copy(u, k).wait_send()
        for k in range(chunks_c):
            c_copy(k, u).wait_send()
    for dz in range(1, lines):
        for k in range(chunks_b):
            b_copy(k, dz).wait_send()
    outs_row = outs_ref.shape[0]
    wide = cols_ref.shape[1] // 128
    picks = {}
    for i in range(rows):
        for k in range(per):
            c = cols_ref[k, base + i]
            safe = jnp.maximum(c, 0)
            for p in range(outs_row):
                o = outs_ref[p, i]
                which = jnp.int32(0)
                hit = jnp.int32(0)
                for j in range(per):
                    match = cols_ref[j, safe] == o
                    which = jnp.where(match, j, which)
                    hit = jnp.where(match & (c >= 0), 1, hit)
                slot = tab[wide_b + wide_c + wide * which + safe // 128, lax.rem(safe, 128)]
                picks[i, k, p] = slot, hit
    for k in range(chunks_c):
        for u in order:
            c_copy(k, u).wait_recv()

    for i in range(rows):
        left = jnp.concatenate([tiles[i, k] for k in range(per)], axis=1)
        stack = []
        for k in range(per):
            line = []
            for p in range(outs_row):
                slot, hit = picks[i, k, p]
                tile = jnp.concatenate([c_recv[s, slot] for s in sources], axis=0)
                line.append(tile * hit.astype(jnp.float32).astype(jnp.bfloat16))
            stack.append(jnp.concatenate(line, axis=1))
        right = jnp.concatenate(stack, axis=0)
        prod = jnp.dot(left, right, preferred_element_type=jnp.float32).astype(jnp.bfloat16)
        for p in range(outs_row):
            out_ref[i, p] = prod[:, p * side : (p + 1) * side]


def params(identity):
    return pltpu.CompilerParams(
        collective_id=identity, has_side_effects=True, vmem_limit_bytes=56 * 1024 * 1024
    )


def shards(block_tiles, tile_columns, requests, output_columns):
    groups = lax.axis_size("grp")
    members = lax.axis_size("row")
    n = groups * members
    rows, per_row, side, _ = block_tiles.shape
    vmem = pl.BlockSpec(memory_space=pltpu.VMEM)
    smem = pl.BlockSpec(memory_space=pltpu.SMEM)
    out = jax.ShapeDtypeStruct((rows, output_columns.shape[1], side, side), jnp.bfloat16)
    tile_rows = lambda count: pltpu.VMEM((count, per_row, side, side), jnp.bfloat16)
    columns, outs = tile_columns.T, output_columns.T

    def dense():
        return pl.pallas_call(
            functools.partial(dense_kernel, groups, members),
            out_shape=out,
            in_specs=[smem, smem, vmem],
            out_specs=vmem,
            scratch_shapes=[
                tile_rows(n),
                tile_rows(n),
                tile_rows(rows),
                pltpu.SemaphoreType.DMA((n,)),
                pltpu.SemaphoreType.DMA((n,)),
                pltpu.SemaphoreType.DMA,
                pltpu.SemaphoreType.DMA,
            ],
            compiler_params=params(0),
        )(columns, outs, block_tiles)

    lines = members // PLANE
    crowd = groups * PLANE
    cap_b, cap_c = CUT_B[-1], CUT_C[-1]
    held = crowd * CUT_A[-1] + (lines - 1) * cap_b
    fits = groups == 2 and members == 4 * PLANE and per_row == 2 and CUT_A[-1] <= 128
    fits = fits and tile_columns.shape[0] % 128 == 0 and side % (16 * crowd) == 0 and held <= 256
    if not fits:
        return dense()
    piece = side // crowd
    pieces = lambda *lead: pltpu.VMEM((*lead, piece, side), jnp.bfloat16)
    dma = pltpu.SemaphoreType.DMA
    hbm = pl.BlockSpec(memory_space=pl.ANY)
    stages, chunks_b, chunks_c = len(CUT_A) - 1, len(CUT_B) - 1, len(CUT_C) - 1
    like = lambda array: jax.ShapeDtypeStruct(array.shape, array.dtype)
    compact, over, columns, outs = pl.pallas_call(
        functools.partial(compact_kernel, groups, members),
        out_shape=(out, jax.ShapeDtypeStruct((1,), jnp.int32), like(columns), like(outs)),
        in_specs=[hbm, hbm, hbm],
        out_specs=(vmem, smem, vmem, vmem),
        scratch_shapes=[
            pltpu.SMEM(columns.shape, jnp.int32),
            pltpu.SMEM(outs.shape, jnp.int32),
            pltpu.VMEM(block_tiles.shape, jnp.bfloat16),
            pltpu.VMEM((CUT_A[-1], side, side), jnp.bfloat16),
            pieces(crowd, CUT_A[-1]),
            pieces(held),
            pieces(lines - 1, cap_b),
            pieces(lines - 1, cap_b),
            pieces(crowd, cap_c),
            pieces(crowd, cap_c),
            pltpu.VMEM((8, 128), jnp.int32),
            pltpu.SMEM((8, 128), jnp.int32),
            pltpu.VMEM((TABLE, 128), jnp.int32),
            pltpu.SMEM((TABLE, 128), jnp.int32),
            dma((5,)),
            dma((2,)),
            dma((stages * crowd,)),
            dma((stages * crowd,)),
            dma((chunks_b * (lines - 1),)),
            dma((chunks_b * (lines - 1),)),
            dma((chunks_c * crowd,)),
            dma((chunks_c * crowd,)),
        ],
        compiler_params=params(1),
    )(columns, outs, block_tiles)
    return lax.cond(over[0] > 0, dense, lambda: compact)


def solution(mesh):
    placed = (
        P(("grp", "row"), None, None, None),
        P(),
        P(("grp", "row"), None),
        P(("grp", "row"), None),
    )
    return jax.shard_map(
        shards,
        mesh=mesh,
        in_specs=placed,
        out_specs=P(("grp", "row"), None, None, None),
        check_vma=False,
    )
```

```python
import functools

import jax
import jax.numpy as jnp
from jax import lax
from jax.experimental import pallas as pl
from jax.experimental.pallas import tpu as pltpu
from jax.sharding import PartitionSpec as P

MESH = pl.DeviceIdType.MESH
PLANE = 4
CUT_A = (0, 2, 6, 12)
START_B = (0, 6, 20)
CUT_B = (0, 6, 20, 32)
CLASS_B = (0, 1, 2)
PART_B = (6, 20)
CUT_C = (0, 2, 6, 15, 20)
SPAN = 40
TABLE = 16


def multiply(base, find, cols_ref, outs_ref, tiles_ref, rbuf, out_ref):
    rows, per_row, side, _ = tiles_ref.shape
    outs_row = outs_ref.shape[0]
    for i in range(rows):
        left = jnp.concatenate([tiles_ref[i, k] for k in range(per_row)], axis=1)
        stack = []
        for k in range(per_row):
            c = cols_ref[k, base + i]
            safe = jnp.maximum(c, 0)
            slot = find(safe // rows)
            line = []
            for p in range(outs_row):
                o = outs_ref[p, i]
                which = jnp.int32(0)
                hit = jnp.int32(0)
                for j in range(per_row):
                    same = cols_ref[j, safe] == o
                    which = jnp.where(same, j, which)
                    hit = jnp.where(same & (c >= 0), 1, hit)
                tile = rbuf[slot, which]
                line.append(tile * hit.astype(jnp.float32).astype(jnp.bfloat16))
            stack.append(jnp.concatenate(line, axis=1))
        right = jnp.concatenate(stack, axis=0)
        prod = jnp.dot(left, right, preferred_element_type=jnp.float32).astype(jnp.bfloat16)
        for p in range(outs_row):
            out_ref[i, p] = prod[:, p * side : (p + 1) * side]


def dense_kernel(
    groups, members, cols_ref, outs_ref, tiles_ref, out_ref,
    sbuf, rbuf, mbuf, send_sem, recv_sem, mirror_send, mirror_recv,
):
    part = members // 2
    n = groups * part
    rows, per_row, side, _ = tiles_ref.shape
    grp, row = lax.axis_index("grp"), lax.axis_index("row")
    half, spot = row // part, lax.rem(row, part)
    me = grp * part + spot
    base = (grp * members + row) * rows
    mirror_row = (1 - half) * part + spot
    mirror = {"grp": grp, "row": mirror_row}
    mirror_base = (grp * members + mirror_row) * rows

    def place(s):
        u = lax.rem(me + s, n)
        return u // part, half * part + lax.rem(u, part)

    def target(s):
        g, r = place(s)
        return {"grp": g, "row": r}

    barrier = pltpu.get_barrier_semaphore()
    pl.semaphore_signal(barrier, inc=1, device_id=mirror, device_id_type=MESH)

    def greet(s, carry):
        pl.semaphore_signal(barrier, inc=1, device_id=target(s), device_id_type=MESH)
        return carry

    lax.fori_loop(1, n, greet, 0)

    def asked(s, start):
        g, r = place(s)
        first = (g * members + r) * rows
        t = jnp.int32(0)
        for i in range(rows):
            for k in range(per_row):
                c = cols_ref[k, first + i] - start
                t = jnp.where((c >= 0) & (c < rows), c, t)
        return t

    def copy(s, level):
        return pltpu.make_async_remote_copy(
            src_ref=sbuf.at[level * n + s],
            dst_ref=rbuf.at[level * n + s],
            send_sem=send_sem.at[level * n + s],
            recv_sem=recv_sem.at[level * n + s],
            device_id=target(s),
            device_id_type=MESH,
        )

    def pack(s, carry):
        sbuf[s] = tiles_ref[asked(s, base)]
        return carry

    lax.fori_loop(1, n, pack, 0)
    pl.semaphore_wait(barrier, n)
    across = pltpu.make_async_remote_copy(
        src_ref=tiles_ref,
        dst_ref=mbuf,
        send_sem=mirror_send,
        recv_sem=mirror_recv,
        device_id=mirror,
        device_id_type=MESH,
    )
    across.start()

    def send(s, carry):
        copy(s, 0).start()
        return carry

    lax.fori_loop(1, n, send, 0)
    rbuf[0] = tiles_ref[asked(0, base)]
    across.wait()

    def relay(s, carry):
        sbuf[n + s] = mbuf[asked(s, mirror_base)]
        return carry

    lax.fori_loop(1, n, relay, 0)

    def forward(s, carry):
        copy(s, 1).start()
        return carry

    lax.fori_loop(1, n, forward, 0)
    rbuf[n] = mbuf[asked(0, mirror_base)]

    def land(s, carry):
        copy(s, 0).wait()
        copy(s, 1).wait()
        return carry

    lax.fori_loop(1, n, land, 0)

    def find(owner):
        owner_row = lax.rem(owner, members)
        spot_of = owner // members * part + lax.rem(owner_row, part)
        return lax.rem(me - spot_of + n, n) + jnp.where(owner_row // part == half, 0, n)

    multiply(base, find, cols_ref, outs_ref, tiles_ref, rbuf, out_ref)


def same(lane, rows, groups, members):
    device = lane // rows
    inner = lax.rem(device, members)
    spot = lax.rem(inner, PLANE)
    return device // members, inner // PLANE, spot // 2, lax.rem(spot, 2)


def ones(mask):
    return jnp.where(mask, 1.0, 0.0)


def across(a, b):
    dims = (((1,), (1,)), ((), ()))
    return lax.dot_general(
        a.astype(jnp.bfloat16), b.astype(jnp.bfloat16), dims, preferred_element_type=jnp.float32
    )


def iota(shape, axis):
    return lax.broadcasted_iota(jnp.int32, shape, axis)


def steps(value, bounds):
    return sum((value >= b).astype(jnp.int32) for b in bounds)


def grouping(total, here, rows, groups, members):
    g, z, y, x = here
    lines = members // PLANE
    crowd = groups * PLANE
    devices = groups * members
    count = devices + 8
    query = iota((count, total), 0)
    lane = iota((count, total), 1)
    og, oz, oy, ox = same(lane, rows, groups, members)
    rel = PLANE * lax.rem(og + g, 2) + 2 * lax.rem(oy + y, 2) + lax.rem(ox + x, 2)
    up = lax.rem(oz - z + lines, lines)
    alone = (query < devices) & (up == query // crowd) & (rel == lax.rem(query, crowd))
    plane = up == query - devices
    return ones(alone | plane).astype(jnp.bfloat16)


def blocks(total, rows):
    a, b = iota((total, total), 0), iota((total, total), 1)
    block = a // rows == b // rows
    return ones(block & (a > b)).astype(jnp.bfloat16), ones(block).astype(jnp.bfloat16)


def named_rows(cols, group):
    total = cols.shape[1]
    index = iota((total, total), 0)
    hits = jnp.zeros((group.shape[0], total), jnp.float32)
    for k in range(cols.shape[0]):
        hits = hits + across(group, ones(index == cols[k : k + 1]))
    return ones(hits > 0.5)


def ranked(masks, upper):
    ranks = []
    before = jnp.zeros((masks[0].shape[0], 1), jnp.float32)
    for m in masks:
        ranks.append(across(m, upper) + before)
        before = before + jnp.sum(m, axis=1, keepdims=True)
    return masks, ranks, before


def slots(held, first, stride, bounds):
    masks, ranks, sums = held
    start = jnp.zeros((8, 1), jnp.float32)
    used, at = [0.0 for _ in masks], [0.0 for _ in masks]
    for k, bound in enumerate(bounds):
        b = 8 * (first + k * stride)
        start = jnp.maximum(start, float(bound))
        for j in range(len(masks)):
            m = masks[j][b : b + 8]
            used[j] = used[j] + m
            at[j] = at[j] + m * (start + ranks[j][b : b + 8])
        start = start + sums[b : b + 8]
    return used, at, start


def triangle(total):
    return ones(iota((total, total), 0) > iota((total, total), 1))


def column(slot, spot, count):
    hot = [ones(slot == spot[q : q + 1]) for q in range(count)]
    return jnp.concatenate(hot, axis=0)


def owned(cols, named, upper, whole, here, rows, groups, members):
    devices = groups * members
    total = cols.shape[1]
    per = cols.shape[0]
    wanted = ones(jnp.sum(named[devices : devices + 8], axis=0, keepdims=True) > 0.5)
    masks = [jnp.broadcast_to(wanted * ones(cols[j : j + 1] >= 0), (8, total)) for j in range(per)]
    ranks = []
    before = jnp.zeros((8, total), jnp.float32)
    for m in masks:
        ranks.append(across(m, upper) + before)
        before = before + across(m, whole)
    lane = iota((8, total), 1)
    og, oz, oy, ox = same(lane, rows, groups, members)
    g, z, y, x = here
    mine = (og == g) & (oz == z) & (oy == y) & (ox == x)
    item = lax.rem(lane, rows)
    picks = jnp.zeros((8, 128), jnp.float32)
    slot = iota((128, total), 0)
    for j in range(per):
        spot = jnp.where(mine & (masks[j] > 0.5), ranks[j], -1.0).astype(jnp.int32)
        picks = picks + across((item * per + j).astype(jnp.float32), column(slot, spot, 1))
    picks = jnp.clip(picks.astype(jnp.int32), 0, rows * per - 1)
    return ranks, before, picks


def tables(cols, named, ranks_a, here, rows, groups, members):
    g, z, y, x = here
    lines = members // PLANE
    crowd = groups * PLANE
    devices = groups * members
    total = cols.shape[1]
    per = cols.shape[0]
    lane = iota((8, total), 1)
    sub = iota((8, total), 0)
    og, oz, oy, ox = same(lane, rows, groups, members)
    rel = PLANE * lax.rem(og + g, 2) + 2 * lax.rem(oy + y, 2) + lax.rem(ox + x, 2)
    local = oz == z
    back = lax.rem(z - oz + lines, lines)
    planes = named[devices : devices + 8]
    mine = jnp.broadcast_to(planes[0:1], (8, total))
    near = named[:crowd]
    upper = triangle(total)
    classes = range(len(START_B))
    present = [ones(cols[j : j + 1] >= 0) for j in range(per)]
    sends, takes = planes * ones(local), mine * ones(back == sub)
    stacks = []
    for j in range(per):
        lev = steps(ranks_a[j], CUT_A[1:-1])
        kept = [present[j] * ones(lev == k) for k in classes]
        stacks.append(jnp.concatenate([sends * m for m in kept] + [takes * m for m in kept], axis=0))
    held = ranked(stacks, upper)
    send_used, send_at, _ = slots(held, 0, 1, START_B)
    take_used, take_at, _ = slots(held, len(classes), 1, START_B)
    cap_a, cap_b, cap_c = CUT_A[-1], CUT_B[-1], CUT_C[-1]
    arena = crowd * cap_a
    first = (rel * cap_a).astype(jnp.float32)
    home = [first + jnp.minimum(ranks_a[j], cap_a - 1.0) for j in range(per)]
    offset = (arena + (sub - 1) * cap_b).astype(jnp.float32)
    arrived, mids = [], []
    for j in range(per):
        spot = jnp.sum(take_used[j] * take_at[j], axis=0, keepdims=True)
        far = jnp.sum(take_used[j] * (offset + take_at[j]), axis=0, keepdims=True)
        arrived.append(jnp.where(local, home[j], jnp.broadcast_to(far, (8, total))))
        part = jnp.where(local, 0, 1 + steps(jnp.broadcast_to(spot, (8, total)), PART_B))
        kept = near * present[j]
        mids.append(jnp.concatenate([kept * ones(part == c) for c in range(len(CUT_C) - 1)], axis=0))
    mid_used, mid_at, _ = slots(ranked(mids, upper), 0, 1, CUT_C[:-1])

    def sources(used, at, address, count):
        out = jnp.zeros((8, SPAN * count), jnp.float32)
        slot = iota((SPAN, total), 0)
        for j in range(per):
            spot = jnp.where(used[j] > 0.5, at[j], -1.0).astype(jnp.int32)
            out = out + across(address[j], column(slot, spot, count))
        return jnp.clip(out.astype(jnp.int32), 0, arena + (lines - 1) * cap_b - 1)

    b_list = sources(send_used, send_at, home, lines)
    c_list = sources(mid_used, mid_at, arrived, crowd)
    final = [jnp.clip(mid_at[j][0:1].astype(jnp.int32), 0, cap_c - 1) for j in range(per)]
    lines_out = []
    for block in [b_list[0:1], c_list[0:1]] + final:
        width = block.shape[1]
        if width % 128:
            block = jnp.concatenate([block, jnp.zeros((1, -width % 128), jnp.int32)], axis=1)
        for h in range(-(-width // 128)):
            lines_out.append(block[:, 128 * h : 128 * h + 128])
    lines_out.append(jnp.zeros((TABLE - len(lines_out), 128), jnp.int32))
    return jnp.concatenate(lines_out, axis=0)


def overflow(cols, named, ranks_a, loads_a, here, rows, groups, members):
    g, z, y, x = here
    lines = members // PLANE
    crowd = groups * PLANE
    devices = groups * members
    total = cols.shape[1]
    per = cols.shape[0]
    lane = iota((8, total), 1)
    oz = lax.rem(lane // rows, members) // PLANE
    up = lax.rem(oz - z + lines, lines)
    planes = named[devices : devices + 8]
    classes = range(len(START_B))
    present = [ones(cols[j : j + 1] >= 0) for j in range(per)]
    stacks = []
    for j in range(per):
        lev = steps(ranks_a[j], CUT_A[1:-1])
        kept = planes * present[j]
        stacks.append(
            jnp.concatenate(
                [kept * ones((up == s) & (lev == k)) for k in classes for s in range(lines)], axis=0
            )
        )
    held = ranked(stacks, triangle(total))
    sub = iota((8, 1), 0)
    worst = jnp.maximum(jnp.max(loads_a, axis=1, keepdims=True) - CUT_A[-1], 0.0)
    at = [0.0 for _ in range(per)]
    for s in range(lines):
        _, spot, end = slots(held, s, lines, START_B)
        worst = jnp.maximum(worst, jnp.where((sub < lines) & (sub != s), end - CUT_B[-1], 0.0))
        for j in range(per):
            at[j] = at[j] + spot[j]
    for q in range(lines):
        near = named[crowd * q : crowd * (q + 1)]
        sums = [jnp.zeros((8, 1), jnp.float32) for _ in CUT_C[:-1]]
        for j in range(per):
            load = near * present[j]
            spot = jnp.broadcast_to(at[j][q : q + 1], (8, total))
            part = jnp.where(up == q, 0, 1 + steps(spot, PART_B))
            for c in range(len(sums)):
                sums[c] = sums[c] + jnp.sum(load * ones(part == c), axis=1, keepdims=True)
        end = jnp.zeros((8, 1), jnp.float32)
        for bound, n in zip(CUT_C, sums):
            end = jnp.maximum(end, float(bound)) + n
        worst = jnp.maximum(worst, end - CUT_C[-1])
    return jnp.max(worst).astype(jnp.int32)


def compact_kernel(
    groups, members, cols_hbm, outs_hbm, tiles_hbm, out_ref, over_ref, cols_vec, outs_vec,
    cols_ref, outs_ref, tiles, a_send, parts, arena, b_send, b_recv, c_send, c_recv,
    own_vec, own, tab_vec, tab, load_sem, tab_sem, a_out, a_in, b_out, b_in, c_out, c_in,
):
    rows, per, side, _ = tiles.shape
    lines = members // PLANE
    crowd = groups * PLANE
    piece = side // crowd
    g, row = lax.axis_index("grp"), lax.axis_index("row")
    z, spot = row // PLANE, lax.rem(row, PLANE)
    y, x = spot // 2, lax.rem(spot, 2)
    here = (g, z, y, x)
    base = (g * members + row) * rows
    me = g * PLANE + spot
    stages, cap_a, cap_b = len(CUT_A) - 1, CUT_A[-1], CUT_B[-1]
    chunks_b, chunks_c = len(CUT_B) - 1, len(CUT_C) - 1

    def near_device(u):
        dg, dy, dx = u // PLANE, u // 2 % 2, u % 2
        ns = 2 * lax.rem(y + dy, 2) + lax.rem(x + dx, 2)
        return {"grp": lax.rem(g + dg, 2), "row": z * PLANE + ns}

    def line_device(dz):
        return {"grp": g, "row": lax.rem(z + dz, lines) * PLANE + spot}

    barrier = pltpu.get_barrier_semaphore()
    for dz in range(1, lines):
        pl.semaphore_signal(barrier, inc=1, device_id=line_device(dz), device_id_type=MESH)
    for u in range(crowd - 1, 0, -1):
        pl.semaphore_signal(barrier, inc=1, device_id=near_device(u), device_id_type=MESH)
    loads = [
        pltpu.make_async_copy(cols_hbm, cols_vec, load_sem.at[0]),
        pltpu.make_async_copy(tiles_hbm, tiles, load_sem.at[1]),
        pltpu.make_async_copy(cols_hbm, cols_ref, load_sem.at[2]),
        pltpu.make_async_copy(outs_hbm, outs_ref, load_sem.at[3]),
        pltpu.make_async_copy(outs_hbm, outs_vec, load_sem.at[4]),
    ]
    for load in loads:
        load.start()
    total = cols_vec.shape[1]
    group = grouping(total, here, rows, groups, members)
    upper, whole = blocks(total, rows)
    loads[0].wait()
    cols = cols_vec[...]
    named = named_rows(cols, group)
    ranks_a, loads_a, picks = owned(cols, named, upper, whole, here, rows, groups, members)
    own_vec[...] = picks
    move = pltpu.make_async_copy(own_vec, own, tab_sem.at[0])
    move.start()
    for load in loads[1:]:
        load.wait()
    move.wait()
    for q in range(cap_a):
        pick = own[0, q]
        tile = tiles[pick // per, lax.rem(pick, per)]
        for part in range(crowd):
            a_send[part, q] = tile[part * piece : part * piece + piece]
    pl.semaphore_wait(barrier, lines - 1 + crowd - 1)

    def a_copy(u, k):
        there = near_device(u)
        part = there["grp"] * PLANE + lax.rem(there["row"], PLANE)
        span = pl.ds(CUT_A[k], CUT_A[k + 1] - CUT_A[k])
        return pltpu.make_async_remote_copy(
            src_ref=a_send.at[part, span],
            dst_ref=parts.at[u, span],
            send_sem=a_out.at[stages * u + k],
            recv_sem=a_in.at[stages * u + k],
            device_id=there,
            device_id_type=MESH,
        )

    order = [7, 3, 5, 6, 1, 2, 4]
    for k in range(stages):
        for u in order:
            a_copy(u, k).start()

    tab_vec[...] = tables(cols, named, ranks_a, here, rows, groups, members)
    move = pltpu.make_async_copy(tab_vec, tab, tab_sem.at[1])
    move.start()
    for q in range(cap_a):
        arena[q] = a_send[me, q]
    move.wait()

    def pick(options):
        value = jnp.int32(options[0])
        for at, option in enumerate(options[1:]):
            value = jnp.where(z == at + 1, option, value)
        return value

    far_first = [pick((3, 2, 2, 1)), pick((2, 1, 3, 2)), pick((1, 3, 1, 3))]

    def b_copy(k, dz):
        span = pl.ds(CUT_B[k], CUT_B[k + 1] - CUT_B[k])
        return pltpu.make_async_remote_copy(
            src_ref=b_send.at[dz - 1, span],
            dst_ref=b_recv.at[dz - 1, span],
            send_sem=b_out.at[chunks_b * (dz - 1) + k],
            recv_sem=b_in.at[chunks_b * (dz - 1) + k],
            device_id=line_device(dz),
            device_id_type=MESH,
        )

    def c_copy(k, u):
        span = pl.ds(CUT_C[k], CUT_C[k + 1] - CUT_C[k])
        return pltpu.make_async_remote_copy(
            src_ref=c_send.at[u, span],
            dst_ref=c_recv.at[u, span],
            send_sem=c_out.at[chunks_c * u + k],
            recv_sem=c_in.at[chunks_c * u + k],
            device_id=near_device(u),
            device_id_type=MESH,
        )

    wide_b, wide_c = -(-lines * SPAN // 128), -(-crowd * SPAN // 128)

    def entry(first, at):
        return tab[first + at // 128, at % 128]

    def push_b(k):
        for dz in range(1, lines):
            for q in range(CUT_B[k], CUT_B[k + 1]):
                b_send[dz - 1, q] = arena[entry(0, SPAN * dz + q)]
        for dz in far_first:
            b_copy(k, dz).start()

    def push_c(k):
        for u in order + [0]:
            for q in range(CUT_C[k], CUT_C[k + 1]):
                tile = arena[entry(wide_b, SPAN * u + q)]
                if u:
                    c_send[u, q] = tile
                else:
                    c_recv[0, q] = tile
        for core in range(groups):
            side_of = PLANE * lax.rem(core - g + groups, groups)
            for at in (3, 1, 2):
                c_copy(k, side_of + at).start()
        c_copy(k, PLANE).start()

    for k in range(stages):
        for u in order:
            a_copy(u, k).wait_recv()
            for q in range(CUT_A[k], CUT_A[k + 1]):
                arena[u * cap_a + q] = parts[u, q]
        for part in range(chunks_b):
            if CLASS_B[part] == k:
                push_b(part)
    push_c(0)
    over_ref[0] = overflow(cols, named, ranks_a, loads_a, here, rows, groups, members)
    held = crowd * cap_a
    sent = 1
    for k in range(chunks_b):
        for dz in range(1, lines):
            b_copy(k, dz).wait_recv()
            for q in range(CUT_B[k], CUT_B[k + 1]):
                arena[held + (dz - 1) * cap_b + q] = b_recv[dz - 1, q]
        if CUT_B[k + 1] in PART_B or k == chunks_b - 1:
            push_c(sent)
            sent += 1

    sources = []
    for piece_of in range(crowd):
        pg, ps = piece_of // PLANE, piece_of % PLANE
        dy, dx = lax.rem(ps // 2 + y, 2), lax.rem(ps % 2 + x, 2)
        sources.append(PLANE * lax.rem(pg + g, 2) + 2 * dy + dx)
    for u in order:
        for k in range(stages):
            a_copy(u, k).wait_send()
        for k in range(chunks_c):
            c_copy(k, u).wait_send()
    for dz in range(1, lines):
        for k in range(chunks_b):
            b_copy(k, dz).wait_send()
    outs_row = outs_ref.shape[0]
    wide = cols_ref.shape[1] // 128
    picks = {}
    for i in range(rows):
        for k in range(per):
            c = cols_ref[k, base + i]
            safe = jnp.maximum(c, 0)
            for p in range(outs_row):
                o = outs_ref[p, i]
                which = jnp.int32(0)
                hit = jnp.int32(0)
                for j in range(per):
                    match = cols_ref[j, safe] == o
                    which = jnp.where(match, j, which)
                    hit = jnp.where(match & (c >= 0), 1, hit)
                slot = tab[wide_b + wide_c + wide * which + safe // 128, lax.rem(safe, 128)]
                picks[i, k, p] = slot, hit
    for k in range(chunks_c):
        for u in order:
            c_copy(k, u).wait_recv()

    for i in range(rows):
        left = jnp.concatenate([tiles[i, k] for k in range(per)], axis=1)
        stack = []
        for k in range(per):
            line = []
            for p in range(outs_row):
                slot, hit = picks[i, k, p]
                tile = jnp.concatenate([c_recv[s, slot] for s in sources], axis=0)
                line.append(tile * hit.astype(jnp.float32).astype(jnp.bfloat16))
            stack.append(jnp.concatenate(line, axis=1))
        right = jnp.concatenate(stack, axis=0)
        prod = jnp.dot(left, right, preferred_element_type=jnp.float32).astype(jnp.bfloat16)
        for p in range(outs_row):
            out_ref[i, p] = prod[:, p * side : (p + 1) * side]


def params(identity):
    return pltpu.CompilerParams(
        collective_id=identity, has_side_effects=True, vmem_limit_bytes=56 * 1024 * 1024
    )


def shards(block_tiles, tile_columns, requests, output_columns):
    groups = lax.axis_size("grp")
    members = lax.axis_size("row")
    n = groups * members
    rows, per_row, side, _ = block_tiles.shape
    vmem = pl.BlockSpec(memory_space=pltpu.VMEM)
    smem = pl.BlockSpec(memory_space=pltpu.SMEM)
    out = jax.ShapeDtypeStruct((rows, output_columns.shape[1], side, side), jnp.bfloat16)
    tile_rows = lambda count: pltpu.VMEM((count, per_row, side, side), jnp.bfloat16)
    columns, outs = tile_columns.T, output_columns.T

    def dense():
        return pl.pallas_call(
            functools.partial(dense_kernel, groups, members),
            out_shape=out,
            in_specs=[smem, smem, vmem],
            out_specs=vmem,
            scratch_shapes=[
                tile_rows(n),
                tile_rows(n),
                tile_rows(rows),
                pltpu.SemaphoreType.DMA((n,)),
                pltpu.SemaphoreType.DMA((n,)),
                pltpu.SemaphoreType.DMA,
                pltpu.SemaphoreType.DMA,
            ],
            compiler_params=params(0),
        )(columns, outs, block_tiles)

    lines = members // PLANE
    crowd = groups * PLANE
    cap_b, cap_c = CUT_B[-1], CUT_C[-1]
    held = crowd * CUT_A[-1] + (lines - 1) * cap_b
    fits = groups == 2 and members == 4 * PLANE and per_row == 2 and CUT_A[-1] <= 128
    fits = fits and tile_columns.shape[0] % 128 == 0 and side % (16 * crowd) == 0 and held <= 256
    if not fits:
        return dense()
    piece = side // crowd
    pieces = lambda *lead: pltpu.VMEM((*lead, piece, side), jnp.bfloat16)
    dma = pltpu.SemaphoreType.DMA
    hbm = pl.BlockSpec(memory_space=pl.ANY)
    stages, chunks_b, chunks_c = len(CUT_A) - 1, len(CUT_B) - 1, len(CUT_C) - 1
    like = lambda array: jax.ShapeDtypeStruct(array.shape, array.dtype)
    compact, over, columns, outs = pl.pallas_call(
        functools.partial(compact_kernel, groups, members),
        out_shape=(out, jax.ShapeDtypeStruct((1,), jnp.int32), like(columns), like(outs)),
        in_specs=[hbm, hbm, hbm],
        out_specs=(vmem, smem, vmem, vmem),
        scratch_shapes=[
            pltpu.SMEM(columns.shape, jnp.int32),
            pltpu.SMEM(outs.shape, jnp.int32),
            pltpu.VMEM(block_tiles.shape, jnp.bfloat16),
            pieces(crowd, CUT_A[-1]),
            pieces(crowd, CUT_A[-1]),
            pieces(held),
            pieces(lines - 1, cap_b),
            pieces(lines - 1, cap_b),
            pieces(crowd, cap_c),
            pieces(crowd, cap_c),
            pltpu.VMEM((8, 128), jnp.int32),
            pltpu.SMEM((8, 128), jnp.int32),
            pltpu.VMEM((TABLE, 128), jnp.int32),
            pltpu.SMEM((TABLE, 128), jnp.int32),
            dma((5,)),
            dma((2,)),
            dma((stages * crowd,)),
            dma((stages * crowd,)),
            dma((chunks_b * (lines - 1),)),
            dma((chunks_b * (lines - 1),)),
            dma((chunks_c * crowd,)),
            dma((chunks_c * crowd,)),
        ],
        compiler_params=params(1),
    )(columns, outs, block_tiles)
    return lax.cond(over[0] > 0, dense, lambda: compact)


def solution(mesh):
    placed = (
        P(("grp", "row"), None, None, None),
        P(),
        P(("grp", "row"), None),
        P(("grp", "row"), None),
    )
    return jax.shard_map(
        shards,
        mesh=mesh,
        in_specs=placed,
        out_specs=P(("grp", "row"), None, None, None),
        check_vma=False,
    )
```
